256 devices in a mesh: slab: 64 (over z, y, core), pencil: 4 (over x).
Axes of the slice: x: 4, y: 4, z: 8, core: 2. Of those that a mesh axis runs over, the one named last changes fastest.
Arguments:
- density_history: float32 [7, 512, 320, 320], P(None, 'slab', 'pencil'), may hold values from -6 to 6
- residual_history: float32 [7, 512, 320, 320], P(None, 'slab', 'pencil'), as said below
- occupancy_history: float32 [7, 6144, 324], P(None, ('slab', 'pencil')), may hold values from -6 to 6
- occupancy_residual: float32 [7, 6144, 324], P(None, ('slab', 'pencil')), may hold values from -6 to 6
- species: int32 [6144], P(('slab', 'pencil')), may hold values from 0 to 3
- slot_count: int32 [256], P(('slab', 'pencil')), may hold values from 12 to 24, as said below
Outputs:
- new_density: float32 [512, 320, 320], P('slab', 'pencil')
- new_occupancy: float32 [6144, 324], P(('slab', 'pencil'))
The draws below stay inside these ranges and needn't reach their ends.
Inputs may be any that keep to these rules, and one draw needn't show every extreme that they name: `residual_history`: residual fields of the 7 previous steps. Device d of slab+pencil (slab slowest) holds slots d * 24 to (d + 1) * 24 - 1, of which the first slot_count[d] hold atoms; some device is full in every draw.
All inputs are finite; a program needn't handle non-finite values.
Results may differ from the reference program's by a relative error of at most 0.00017.
Values sent between devices are 32-bit elements; how exact they have to be, the bound alone decides.
A program may use at most 128 MiB of HBM per device.

```python
import math
import jax
import jax.numpy as jnp
from jax import lax

HISTORY = 7
NX = 320
NY = 320
NZ = 512
ORBITALS = 18
SLOT_DEV = 24
SLOTS = 6144


def smooth_lines(key, leading, length):
    keys = jax.random.split(key, 2)
    amplitude = 0.5 * jax.random.normal(keys[0], leading + (4,), jnp.float32)
    phase = jax.random.uniform(keys[1], leading + (4,), jnp.float32, 0.0, 2.0 * math.pi)
    position = jnp.arange(length, dtype=jnp.float32)
    wavenumber = jnp.arange(1, 5, dtype=jnp.float32)
    angle = 2.0 * math.pi * wavenumber[:, None] * position[None, :] / length
    return jnp.sum(amplitude[..., None] * jnp.cos(angle + phase[..., None]), axis=-2)


def region_scale(key, length, upper):
    return jnp.exp(jax.random.uniform(key, (length,), jnp.float32, 0.0, math.log(upper)))


def draw_residual_history(key, part):
    keys = jax.random.split(key, 11)
    shared = 0.6
    spread = 4.0
    upper = 3.0
    common_noise = jax.random.normal(keys[0], (NZ, NY, NX), jnp.float32)
    own_noise = jax.random.normal(keys[1], (HISTORY, NZ, NY, NX), jnp.float32)
    region = region_scale(keys[2], NZ, upper)[:, None, None] * region_scale(keys[3], NY, upper)[None, :, None] * region_scale(keys[4], NX, upper)[None, None, :]
    common_smooth = smooth_lines(keys[5], (), NZ)[:, None, None] + smooth_lines(keys[6], (), NY)[None, :, None] + smooth_lines(keys[7], (), NX)[None, None, :]
    own_smooth = smooth_lines(keys[8], (HISTORY,), NZ)[:, :, None, None] + smooth_lines(keys[9], (HISTORY,), NY)[:, None, :, None] + smooth_lines(keys[10], (HISTORY,), NX)[:, None, None, :]
    common = common_noise * region + common_smooth
    own = own_noise * region[None] + own_smooth
    step_index = jnp.arange(HISTORY, dtype=jnp.float32)
    history_scale = jnp.exp(math.log(spread) * (1.0 - step_index / max(HISTORY - 1, 1)))
    value = history_scale[:, None, None, None] * (shared * common[None] + math.sqrt(1.0 - shared * shared) * own)
    return value.astype(jnp.float32)


def draw_slot_count(key, part):
    keys = jax.random.split(key, 2)
    devices_total = SLOTS // SLOT_DEV
    counts = jax.random.randint(keys[0], (devices_total,), max(1, SLOT_DEV // 2), SLOT_DEV + 1)
    filled = jax.random.randint(keys[1], (), 0, devices_total)
    position = jnp.arange(devices_total, dtype=jnp.int32)
    return jnp.where(position == filled, SLOT_DEV, counts).astype(jnp.int32)


def set_ends(result, stream_key, least, top_value):
    spot = [jax.random.randint(jax.random.fold_in(stream_key, axis), (), 0, length) for axis, length in enumerate(result.shape)]
    main_axis = result.shape.index(max(result.shape))
    next_to = spot[:main_axis] + [(spot[main_axis] + 1) % result.shape[main_axis]] + spot[main_axis + 1:]
    return result.at[tuple(spot)].set(least).at[tuple(next_to)].set(top_value)


def block_levels(key, shape, cuts, least, largest):
    gain = 1.0
    for axis_at, parts in cuts:
        draws = jax.random.uniform(jax.random.fold_in(jax.random.fold_in(key, 6), axis_at), (parts,), jnp.float32, least / len(cuts), largest / len(cuts))
        gain = gain * jnp.repeat(jnp.exp(draws), shape[axis_at] // parts).reshape((-1,) + (1,) * (len(shape) - 1 - axis_at))
    return gain


def gaussian(key, shape, width, reach, cuts=(), kind=jnp.bfloat16):
    drawn = jax.random.normal(key, shape, jnp.float32) * width
    if len(cuts) > 0:
        drawn = block_levels(key, shape, cuts, -0.22, 0.18) * drawn
    return jnp.clip(drawn, min=-reach, max=reach).astype(kind)


def setup_inputs(seed: int = 0) -> dict:
    key_of = jax.random.split(jax.random.key(seed), 7)
    return {
        "density_history": gaussian(key_of[0], (HISTORY, NZ, NY, NX), 1.0, 6.0, ((1, 64), (2, 4)), jnp.float32),
        "residual_history": draw_residual_history(jax.random.fold_in(key_of[6], 71), 0),
        "occupancy_history": gaussian(key_of[2], (HISTORY, SLOTS, ORBITALS * ORBITALS), 1.0, 6.0, ((1, 256),), jnp.float32),
        "occupancy_residual": gaussian(key_of[3], (HISTORY, SLOTS, ORBITALS * ORBITALS), 1.0, 6.0, ((1, 256),), jnp.float32),
        "species": set_ends(jax.random.randint(key_of[4], (SLOTS,), 0, 4), jax.random.fold_in(key_of[4], 1), 0, 3).astype(jnp.int32),
        "slot_count": draw_slot_count(jax.random.fold_in(key_of[6], 71), 0),
    }


highest = lax.Precision.HIGHEST
grid_mixing = 0.5
block_mixing = 0.5
kerker_wave = 6.0
species_orbitals = (18, 13, 8, 5)

def block_mask(species, slot_count):
    position = jnp.arange(species.shape[0], dtype=jnp.int32)
    owner_count = slot_count[(position // SLOT_DEV).astype(jnp.int32)]
    live = position % SLOT_DEV < owner_count
    orbitals = jnp.zeros_like(species)
    for species_index, orbital_number in enumerate(species_orbitals):
        orbitals = orbitals + orbital_number * (species == species_index).astype(jnp.int32)
    entry = jnp.arange(ORBITALS * ORBITALS, dtype=jnp.int32)
    row_index = entry // ORBITALS
    column_index = entry % ORBITALS
    inside = (row_index[None, :] < orbitals[:, None]) & (column_index[None, :] < orbitals[:, None]) & live[:, None]
    return inside.astype(jnp.float32)

def mixing_weights(intersection):
    factor = jnp.linalg.cholesky(intersection)
    column = jnp.ones((intersection.shape[0], 1), intersection.dtype)
    middle = lax.linalg.triangular_solve(factor, column, left_side=True, lower=True)
    solved = lax.linalg.triangular_solve(factor, middle, left_side=True, lower=True, transpose_a=True)
    return solved[:, 0] / jnp.sum(solved)

def magnitude(length):
    index = jnp.arange(length, dtype=jnp.int32)
    return jnp.minimum(index, length - index).astype(jnp.float32)

def reference(density_history, residual_history, occupancy_history, occupancy_residual, species, slot_count):
    mask = block_mask(species, slot_count)
    flat = residual_history.reshape(HISTORY, -1)
    grid_intersection = jnp.dot(flat, flat.T, precision=highest) / (NX * NY * NZ)
    blocks = (occupancy_residual * mask[None]).reshape(HISTORY, -1)
    block_intersection = jnp.dot(blocks, blocks.T, precision=highest) / (100.0 * SLOTS)
    weights = mixing_weights(grid_intersection + block_intersection)
    mixed = jnp.tensordot(weights, residual_history, axes=1, precision=highest)
    spectrum = jnp.fft.fftn(mixed)
    square = magnitude(NZ)[:, None, None] ** 2 + magnitude(NY)[None, :, None] ** 2 + magnitude(NX)[None, None, :] ** 2
    factor = square / (square + kerker_wave * kerker_wave)
    filtered = jnp.real(jnp.fft.ifftn(spectrum * factor)).astype(jnp.float32)
    new_density = jnp.tensordot(weights, density_history, axes=1, precision=highest) + grid_mixing * filtered
    mixed_blocks = jnp.tensordot(weights, occupancy_history + block_mixing * occupancy_residual, axes=1, precision=highest)
    return (new_density, mask * mixed_blocks)
```

```python
import functools
import math

import numpy as np

import jax
import jax.numpy as jnp
from jax import lax
from jax.experimental import pallas as pl
from jax.experimental.pallas import tpu as pltpu
from jax.sharding import Mesh
from jax.sharding import PartitionSpec as P

ORBITALS = 18
SLAB = ("slab_0", "slab_1", "slab_2")
SLAB_PENCIL = ("slab_0", "slab_1", "slab_2", "pencil")

grid_mixing = 0.5
block_mixing = 0.5
kerker_wave = 6.0
species_orbitals = (18, 13, 8, 5)


def real_basis(length):
    half = length // 2
    n = np.arange(length)
    rows = [np.full(length, 1.0 / math.sqrt(length))]
    waves = [0]
    for k in range(1, half):
        angle = 2.0 * math.pi * ((k * n) % length) / length
        rows.append(math.sqrt(2.0 / length) * np.cos(angle))
        rows.append(math.sqrt(2.0 / length) * np.sin(angle))
        waves += [k, k]
    rows.append(np.where(n % 2 == 0, 1.0, -1.0) / math.sqrt(length))
    waves.append(half)
    return np.stack(rows).astype(np.float32), np.array(waves, np.float32)


def block_mask(species, slot_count):
    live = jnp.arange(species.shape[0], dtype=jnp.int32) < slot_count[0]
    orbitals = jnp.zeros_like(species)
    for species_index, orbital_number in enumerate(species_orbitals):
        orbitals = orbitals + orbital_number * (species == species_index).astype(jnp.int32)
    entry = jnp.arange(ORBITALS * ORBITALS, dtype=jnp.int32)
    row_index = entry // ORBITALS
    column_index = entry % ORBITALS
    inside = (
        (row_index[None, :] < orbitals[:, None])
        & (column_index[None, :] < orbitals[:, None])
        & live[:, None]
    )
    return inside.astype(jnp.float32)


def mixing_weights(intersection):
    factor = jnp.linalg.cholesky(intersection)
    column = jnp.ones((intersection.shape[0], 1), intersection.dtype)
    middle = lax.linalg.triangular_solve(factor, column, left_side=True, lower=True)
    solved = lax.linalg.triangular_solve(
        factor, middle, left_side=True, lower=True, transpose_a=True
    )
    return solved[:, 0] / jnp.sum(solved)


def gram_kernel(history, pairs, field_ref, out_ref):
    rows = field_ref.shape[2]

    def step(r, acc):
        at = pl.multiple_of(r * 8, 8)
        acc = list(acc)
        for lanes in ((0, 128), (128, 128)):
            v = [field_ref[i, 0, pl.ds(at, 8), lanes[0] : lanes[0] + lanes[1]] for i in range(history)]
            for n, (i, j) in enumerate(pairs):
                acc[n] = acc[n] + v[i] * v[j]
        v = [field_ref[i, 0, pl.ds(at, 8), 256:320] for i in range(history)]
        v = [jnp.concatenate([x, jnp.zeros_like(x)], axis=1) for x in v]
        for n, (i, j) in enumerate(pairs):
            acc[n] = acc[n] + v[i] * v[j]
        return tuple(acc)

    zero = jnp.zeros((8, 128), jnp.float32)
    acc = lax.fori_loop(0, rows // 8, step, (zero,) * len(pairs))

    @pl.when(pl.program_id(0) == 0)
    def _():
        for n in range(len(pairs)):
            out_ref[n] = acc[n]

    @pl.when(pl.program_id(0) > 0)
    def _():
        for n in range(len(pairs)):
            out_ref[n] += acc[n]


def gram_partial(field):
    history, planes, rows, columns = field.shape
    pairs = [(i, j) for i in range(history) for j in range(i + 1)]
    out = pl.pallas_call(
        functools.partial(gram_kernel, history, pairs),
        grid=(planes,),
        in_specs=[pl.BlockSpec((history, 1, rows, columns), lambda z: (0, z, 0, 0))],
        out_specs=pl.BlockSpec((len(pairs), 8, 128), lambda z: (0, 0, 0)),
        out_shape=jax.ShapeDtypeStruct((len(pairs), 8, 128), jnp.float32),
    )(field)
    flat = jnp.sum(out, axis=(1, 2))
    index = np.zeros((history, history), np.int32)
    for n, (i, j) in enumerate(pairs):
        index[i, j] = index[j, i] = n
    select = np.zeros((history * history, len(pairs)), np.float32)
    select[np.arange(history * history), index.reshape(-1)] = 1.0
    return jnp.sum(select * flat[None, :], axis=1).reshape(history, history)


def mix_kernel(history, weights_ref, field_ref, *rest):
    out_ref = rest[-1]
    total = weights_ref[0] * field_ref[0]
    for i in range(1, history):
        total += weights_ref[i] * field_ref[i]
    if len(rest) == 2:
        total += grid_mixing * rest[0][...]
    out_ref[...] = total


def mix(weights, field, extra=None):
    history, planes, rows, columns = field.shape
    plane = pl.BlockSpec((1, rows, columns), lambda z: (z, 0, 0))
    args = (weights, field) + (() if extra is None else (extra,))
    return pl.pallas_call(
        functools.partial(mix_kernel, history),
        grid=(planes,),
        in_specs=[
            pl.BlockSpec(memory_space=pltpu.SMEM),
            pl.BlockSpec((history, 1, rows, columns), lambda z: (0, z, 0, 0)),
        ]
        + [plane] * (len(args) - 2),
        out_specs=plane,
        out_shape=jax.ShapeDtypeStruct((planes, rows, columns), jnp.float32),
    )(*args)


def body(
    density_history, residual_history, occupancy_history, occupancy_residual, species, slot_count
):
    histories, z_local, y_local, x_length = residual_history.shape
    slabs = lax.axis_size(SLAB)
    pencils = lax.axis_size("pencil")
    y_length = y_local * pencils
    z_length = z_local * slabs
    kx_local = x_length // pencils
    ky_local = y_length // slabs
    cells = z_length * y_length * x_length
    slot_total = species.shape[0] * slabs * pencils
    mask = block_mask(species, slot_count)
    grid_local = gram_partial(residual_history) / cells
    blocks = occupancy_residual * mask[None]
    block_local = jnp.sum(blocks[:, None] * blocks[None, :], axis=(2, 3)) / (100.0 * slot_total)
    weights = mixing_weights(lax.psum(grid_local + block_local, SLAB_PENCIL))
    mixed = mix(weights, residual_history)

    high = lax.Precision.HIGH
    qx, wx = real_basis(x_length)
    qy, wy = real_basis(y_length)
    qz, wz = real_basis(z_length)
    h = jnp.einsum("kx,zyx->kzy", qx, mixed, precision=high).reshape(pencils, -1)
    h = lax.all_to_all(h, "pencil", split_axis=0, concat_axis=0, tiled=True)
    h = h.reshape(pencils, kx_local, z_local, y_local)
    h = jnp.einsum("lqy,qkzy->lkz", qy.reshape(y_length, pencils, y_local), h, precision=high)
    h = lax.all_to_all(h.reshape(slabs, -1), SLAB, split_axis=0, concat_axis=0, tiled=True)
    h = h.reshape(slabs, ky_local, kx_local, z_local)
    qz3 = qz.reshape(z_length, slabs, z_local)
    h = jnp.einsum("msz,slkz->mlk", qz3, h, precision=high)
    own_x = lax.dynamic_slice_in_dim(jnp.asarray(wx), lax.axis_index("pencil") * kx_local, kx_local)
    own_y = lax.dynamic_slice_in_dim(jnp.asarray(wy), lax.axis_index(SLAB) * ky_local, ky_local)
    square = (wz**2)[:, None, None] + (own_y**2)[None, :, None] + (own_x**2)[None, None, :]
    h = h * (square / (square + kerker_wave * kerker_wave))
    h = jnp.einsum("msz,mlk->slkz", qz3, h, precision=high)
    h = lax.all_to_all(h.reshape(slabs, -1), SLAB, split_axis=0, concat_axis=0, tiled=True)
    h = h.reshape(y_length, kx_local, z_local)
    h = jnp.einsum("lqy,lkz->qkzy", qy.reshape(y_length, pencils, y_local), h, precision=high)
    h = lax.all_to_all(h.reshape(pencils, -1), "pencil", split_axis=0, concat_axis=0, tiled=True)
    h = h.reshape(x_length, z_local, y_local)
    filtered = jnp.einsum("kx,kzy->zyx", qx, h, precision=high)
    new_density = mix(weights, density_history, filtered)
    mixed_blocks = jnp.sum(
        weights[:, None, None] * (occupancy_history + block_mixing * occupancy_residual), axis=0
    )
    return (new_density, mask * mixed_blocks)


def solution(mesh):
    torus = Mesh(
        mesh.devices.reshape(8, 4, 2, mesh.shape["pencil"]),
        ("slab_0", "slab_1", "slab_2", "pencil"),
    )
    placed = (
        P(None, SLAB, "pencil", None),
        P(None, SLAB, "pencil", None),
        P(None, SLAB_PENCIL, None),
        P(None, SLAB_PENCIL, None),
        P(SLAB_PENCIL),
        P(SLAB_PENCIL),
    )
    return jax.shard_map(
        body,
        mesh=torus,
        in_specs=placed,
        out_specs=(P(SLAB, "pencil", None), P(SLAB_PENCIL, None)),
        check_vma=False,
    )
```

```python
import functools
import math

import numpy as np

import jax
import jax.numpy as jnp
from jax import lax
from jax.experimental import pallas as pl
from jax.experimental.pallas import tpu as pltpu
from jax.sharding import Mesh
from jax.sharding import PartitionSpec as P

ORBITALS = 18
SLAB = ("slab_0", "slab_1", "slab_2")
SLAB_PENCIL = ("slab_0", "slab_1", "slab_2", "pencil")
MESH = pl.DeviceIdType.MESH

grid_mixing = 0.5
block_mixing = 0.5
kerker_wave = 6.0
species_orbitals = (18, 13, 8, 5)

H = 7
SLABS = 64
PENCILS = 4
ZL = 8
YL = 80
NX = 320
NY = YL * PENCILS
NZ = ZL * SLABS
KY = NY // SLABS
LT = 5
WIDE = 64
NARROW = 16
PAIRS = [(i, j) for i in range(H) for j in range(i + 1)]


def real_basis(length):
    half = length // 2
    n = np.arange(length)
    rows = [np.full(length, 1.0 / math.sqrt(length))]
    for k in range(1, half):
        angle = 2.0 * math.pi * ((k * n) % length) / length
        rows.append(math.sqrt(2.0 / length) * np.cos(angle))
        rows.append(math.sqrt(2.0 / length) * np.sin(angle))
    rows.append(np.where(n % 2 == 0, 1.0, -1.0) / math.sqrt(length))
    return np.stack(rows)


def two_parts(table):
    upper = table.astype(np.float32).astype(jnp.bfloat16)
    lower = (table - upper.astype(np.float64)).astype(np.float32).astype(jnp.bfloat16)
    return upper, lower


def block_mask(species, slot_count):
    live = jnp.arange(species.shape[0], dtype=jnp.int32) < slot_count[0]
    orbitals = jnp.zeros_like(species)
    for species_index, orbital_number in enumerate(species_orbitals):
        orbitals = orbitals + orbital_number * (species == species_index).astype(jnp.int32)
    entry = jnp.arange(ORBITALS * ORBITALS, dtype=jnp.int32)
    row_index = entry // ORBITALS
    column_index = entry % ORBITALS
    inside = (
        (row_index[None, :] < orbitals[:, None])
        & (column_index[None, :] < orbitals[:, None])
        & live[:, None]
    )
    return inside.astype(jnp.float32)


def split(value):
    upper = value.astype(jnp.bfloat16)
    lower = (value - upper.astype(jnp.float32)).astype(jnp.bfloat16)
    return upper, lower


def dot3(ah, al, bh, bl):
    dot = functools.partial(jnp.dot, preferred_element_type=jnp.float32)
    return dot(ah, bh) + (dot(ah, bl) + dot(al, bh))


def lanes_of(shape):
    return lax.broadcasted_iota(jnp.int32, shape, 1)


def swap(a, b):
    low = lanes_of(a.shape) < 64
    return (
        jnp.where(low, a, pltpu.roll(b, 64, 1)),
        jnp.where(low, pltpu.roll(a, 64, 1), b),
    )


def regroup(pieces, place):
    lane = lanes_of(pieces[0].shape)
    total = jnp.zeros_like(pieces[0])
    for n, piece in enumerate(pieces):
        shift = (16 * (n - place)) % 128
        moved = pltpu.roll(piece, shift, 1) if shift else piece
        total = jnp.where((lane >= 16 * n) & (lane < 16 * n + 16), moved, total)
    return total


def kernel(
    res, den, occ_h, occ_r, mask, t0, t1, t2, t3, t4, t5, t6, t7,
    out, occ_out,
    r7, d7, tx0, tx1, tx2, tx3, tz0, tz1, tz2, tz3,
    row_mine, row_pencil, row_group, row_slab, weight,
    mh, ml, hs, xs, yin, ys, zin, zh, zl, fac, zu, zout, yb, yo, xi, dm,
    load_sem, table_sem, send_sem, recv_sem,
):
    s0, s1, s2 = (lax.axis_index(a) for a in SLAB)
    me_p = lax.axis_index("pencil")
    me_s = (s0 * 4 + s1) * 2 + s2

    def slab_at(r):
        t = lax.rem(me_s + r, SLABS)
        return t, (t // 8, lax.rem(t // 2, 4), lax.rem(t, 2), me_p)

    def pencil_at(r):
        q = lax.rem(me_p + r, PENCILS)
        return q, (s0, s1, s2, q)

    loads = []
    for z in range(ZL):
        rows = pl.ds(z * YL, YL)
        loads.append(pltpu.make_async_copy(res.at[:, rows], r7.at[:, rows], load_sem.at[z]))
    for c in loads:
        c.start()
    tables = []
    for n, (a, b) in enumerate(
        zip((t0, t1, t2, t3, t4, t5, t6, t7), (tx0, tx1, tx2, tx3, tz0, tz1, tz2, tz3))
    ):
        tables.append(pltpu.make_async_copy(a, b, table_sem.at[n]))
    tables.append(pltpu.make_async_copy(den, d7, table_sem.at[8]))

    barrier = pltpu.get_barrier_semaphore()
    for r in range(1, PENCILS):
        pl.semaphore_signal(barrier, inc=1, device_id=pencil_at(r)[1], device_id_type=MESH)

    def greet(r, c):
        pl.semaphore_signal(barrier, inc=1, device_id=slab_at(r)[1], device_id_type=MESH)
        return c

    lax.fori_loop(1, SLABS, greet, 0)

    zero = jnp.zeros((8, 128), jnp.float32)

    def add_products(acc, v):
        return [acc[n] + v[i] * v[j] for n, (i, j) in enumerate(PAIRS)]

    def pad(v):
        return jnp.concatenate([v, jnp.zeros((8, 128 - v.shape[1]), v.dtype)], axis=1)

    def block_step(r, acc):
        at = pl.ds(pl.multiple_of(r * 8, 8), 8)
        acc = list(acc)
        for lo, hi in ((0, 128), (128, 256), (256, 324)):
            m = mask[at, lo:hi]
            v = [occ_r[i, at, lo:hi] * m for i in range(H)]
            acc = add_products(acc, v if hi - lo == 128 else [pad(x) for x in v])
        return tuple(acc)

    block = lax.fori_loop(0, 3, block_step, (zero,) * len(PAIRS))
    cells = NX * NY * NZ
    scale = cells / (100.0 * SLABS * PENCILS * mask.shape[0])
    acc = tuple(x * scale for x in block)

    def grid_step(r, acc):
        at = pl.ds(pl.multiple_of(r * 8, 8), 8)
        acc = list(acc)
        for lo, hi in ((0, 128), (128, 256), (256, 320)):
            v = [r7[i, at, lo:hi] for i in range(H)]
            acc = add_products(acc, v if hi - lo == 128 else [pad(x) for x in v])
        return tuple(acc)

    for z in range(ZL):
        loads[z].wait()
        acc = lax.fori_loop(z * 10, z * 10 + 10, grid_step, acc)
    for c in tables:
        c.start()

    lane = lanes_of((8, 128))
    sub = lax.broadcasted_iota(jnp.int32, (8, 128), 0)
    spread = zero
    for n0 in range(0, len(PAIRS), 8):
        tile = zero
        for r, x in enumerate(acc[n0 : n0 + 8]):
            tile = jnp.where(sub == r, jnp.sum(x, axis=0, keepdims=True), tile)
        column = jnp.sum(tile, axis=1, keepdims=True)
        for r, (i, j) in enumerate(PAIRS[n0 : n0 + 8]):
            here = (sub == r) & ((lane == 8 * i + j) | (lane == 8 * j + i))
            spread = jnp.where(here, column, spread)
    row_mine[0] = jnp.sum(spread, axis=0, keepdims=True)

    pl.semaphore_wait(barrier, PENCILS - 1 + SLABS - 1)

    def exchange(phase, source_at, target, me, at, count, unroll):
        def copy(r):
            q, device = at(r)
            return pltpu.make_async_remote_copy(
                src_ref=source_at(q),
                dst_ref=target(me),
                send_sem=send_sem.at[phase],
                recv_sem=recv_sem.at[phase],
                device_id=device,
                device_id_type=MESH,
            )

        if unroll:
            for r in range(1, count):
                copy(r).start()
        else:
            lax.fori_loop(1, count, lambda r, c: (copy(r).start(), c)[1], 0)
        pltpu.make_async_copy(source_at(me), target(me), recv_sem.at[phase]).start()

        def finish():
            if unroll:
                for r in range(1, count):
                    copy(r).wait_send()
            else:
                lax.fori_loop(1, count, lambda r, c: (copy(r).wait_send(), c)[1], 0)

        return finish

    def arrive(phase, whole):
        pltpu.make_async_copy(whole, whole, recv_sem.at[phase]).wait()

    done = []
    done.append(
        exchange(
            0, lambda q: row_mine.at[0], lambda m: row_pencil.at[m], me_p, pencil_at, PENCILS, True
        )
    )
    arrive(0, row_pencil)
    row_group[0] = (row_pencil[0] + row_pencil[1]) + (row_pencil[2] + row_pencil[3])
    done.append(
        exchange(
            1, lambda q: row_group.at[0], lambda m: row_slab.at[m], me_s, slab_at, SLABS, False
        )
    )
    arrive(1, row_slab)
    total = row_slab.reshape(SLABS, 128)[...]
    total = jnp.sum(total, axis=0, keepdims=True) * (1.0 / cells)

    m = zero
    for i in range(H):
        m = jnp.where(sub == i, pltpu.roll(total, (128 - 8 * i) % 128, 1) if i else total, m)
    m = jnp.where(lane < H, m, 0.0)
    m = jnp.where((lane == H) & (sub < H), 1.0, m)
    for k in range(H):
        pivot_row = m[k : k + 1, :] / m[k : k + 1, k : k + 1]
        m = jnp.where(sub == k, pivot_row, m - m[:, k : k + 1] * pivot_row)
    solved = m[:, H : H + 1]
    weight[...] = jnp.broadcast_to(solved / jnp.sum(solved, axis=0, keepdims=True), (8, 128))

    w320 = [
        jnp.broadcast_to(weight[i : i + 1, 0:1], (16, NX)) for i in range(H)
    ]

    def mix_step(r, c):
        at = pl.ds(pl.multiple_of(r * 16, 16), 16)
        v = w320[0] * r7[0, at]
        for i in range(1, H):
            v += w320[i] * r7[i, at]
        mh[at, :], ml[at, :] = split(v)
        return c

    lax.fori_loop(0, ZL * YL // 16, mix_step, 0)
    for c in tables[:4]:
        c.wait()

    def x_step(j, c):
        at = pl.ds(pl.multiple_of(j * 160, 160), 160)
        h = dot3(mh[at, :], ml[at, :], tx2[...], tx3[...])
        hs[at, 0:256] = h[:, 0:256]
        hs[at, 256:384] = jnp.concatenate(
            [h[:, 256:320], jnp.zeros((160, 64), jnp.float32)], axis=1
        )
        return c

    lax.fori_loop(0, 4, x_step, 0)
    for j in range(4):
        for c in range(2):
            a = hs[2 * j * YL : (2 * j + 1) * YL, 128 * c : 128 * c + 128]
            b = hs[(2 * j + 1) * YL : (2 * j + 2) * YL, 128 * c : 128 * c + 128]
            xs[2 * c, j], xs[2 * c + 1, j] = swap(a, b)
    for b in range(PENCILS):
        xs[b, 4] = regroup([hs[z * YL : (z + 1) * YL, 256:384] for z in range(ZL)], b)
    done.append(
        exchange(2, lambda q: xs.at[q], lambda m: yin.at[m], me_p, pencil_at, PENCILS, True)
    )

    def factor_step(r, c):
        at = pl.ds(pl.multiple_of(r * 8, 8), 8)
        kz = (lax.broadcasted_iota(jnp.int32, (8, 512), 0) + r * 8 + 1) // 2
        line = lanes_of((8, 512))
        wide = line < 384
        within = line - 384
        kx = jnp.where(wide, me_p * WIDE + lax.rem(line, 64), 256 + me_p * NARROW + lax.rem(within, 16))
        ky = me_s * KY + jnp.where(wide, line // 64, within // 16)
        kx = (kx + 1) // 2
        ky = (ky + 1) // 2
        square = (kz * kz + ky * ky + kx * kx).astype(jnp.float32)
        fac[at, :] = square / (square + kerker_wave * kerker_wave)
        return c

    lax.fori_loop(0, NZ // 8, factor_step, 0)

    for lo, hi in ((0, 128), (128, 256), (256, 324)):
        v = jnp.zeros((24, hi - lo), jnp.float32)
        for i in range(H):
            w = jnp.broadcast_to(weight[i : i + 1, 0:1], (24, hi - lo))
            v += w * (occ_h[i, :, lo:hi] + block_mixing * occ_r[i, :, lo:hi])
        occ_out[:, lo:hi] = mask[:, lo:hi] * v

    arrive(2, yin)

    y = jnp.concatenate([yin[:, n].reshape(NY, 128) for n in range(LT)], axis=1)
    yh, yl = split(y)
    y = dot3(tx0[...], tx1[...], yh, yl)
    for n in range(LT):
        ys[n] = y[:, 128 * n : 128 * n + 128]
    ys_rows = ys.reshape(LT, NY, 1, 128)
    zin_rows = zin.reshape(LT, KY, SLABS, 1, 128)
    done.append(
        exchange(
            3,
            lambda q: ys_rows.at[:, pl.ds(q * KY, KY)],
            lambda m: zin_rows.at[:, :, m],
            me_s, slab_at, SLABS, False,
        )
    )

    for c in tables[4:]:
        c.wait()

    def density_step(r, c):
        at = pl.ds(pl.multiple_of(r * 16, 16), 16)
        v = w320[0] * d7[0, at]
        for i in range(1, H):
            v += w320[i] * d7[i, at]
        dm[at, :] = v
        return c

    lax.fori_loop(0, ZL * YL // 16, density_step, 0)
    arrive(3, zin)

    def put(z, tile, value):
        at = slice(64 * z, 64 * z + 64)
        lanes = slice(128 * tile, 128 * tile + 128)
        zh[at, lanes], zl[at, lanes] = split(value)

    for j in range(4):
        for tile, ky in ((0, 0), (1, 2), (2, 4)):
            a, b = swap(zin[j, ky], zin[j, min(ky + 1, 4)])
            put(2 * j, tile, a)
            put(2 * j + 1, tile, b)
    for z in range(ZL):
        put(z, 3, regroup([zin[4, ky] for ky in range(KY)], z))
    for n in range(2):
        lanes = slice(256 * n, 256 * n + 256)
        u = dot3(tz0[...], tz1[...], zh[:, lanes], zl[:, lanes])
        zu[:, lanes] = u * fac[:, lanes]
    for r in range(8):
        at = slice(64 * r, 64 * r + 64)
        zh[at, :], zl[at, :] = split(zu[at, :])
    for n in range(2):
        lanes = slice(256 * n, 256 * n + 256)
        zu[:, lanes] = dot3(tz2[...], tz3[...], zh[:, lanes], zl[:, lanes])

    def got(z, tile):
        return zu[64 * z : 64 * z + 64, 128 * tile : 128 * tile + 128]

    for j in range(4):
        for tile, ky in ((0, 0), (1, 2), (2, 4)):
            a, b = swap(got(2 * j, tile), got(2 * j + 1, tile))
            zout[j, ky] = a
            if ky < 4:
                zout[j, ky + 1] = b
    for ky in range(KY):
        zout[4, ky] = regroup([got(z, 3) for z in range(ZL)], ky)
    zout_rows = zout.reshape(LT, KY, SLABS, 1, 128)
    yb_rows = yb.reshape(LT, NY, 1, 128)
    done.append(
        exchange(
            4,
            lambda q: zout_rows.at[:, :, q],
            lambda m: yb_rows.at[:, pl.ds(m * KY, KY)],
            me_s, slab_at, SLABS, False,
        )
    )
    arrive(4, yb)

    y = jnp.concatenate([yb[n] for n in range(LT)], axis=1)
    yh, yl = split(y)
    y = dot3(tx2[...], tx3[...], yh, yl)
    for n in range(LT):
        yo[:, n] = y[:, 128 * n : 128 * n + 128].reshape(PENCILS, YL, 128)
    done.append(
        exchange(5, lambda q: yo.at[q], lambda m: xi.at[m], me_p, pencil_at, PENCILS, True)
    )
    arrive(5, xi)

    for j in range(4):
        for c in range(2):
            a, b = swap(xi[2 * c, j], xi[2 * c + 1, j])
            hs[2 * j * YL : (2 * j + 1) * YL, 128 * c : 128 * c + 128] = a
            hs[(2 * j + 1) * YL : (2 * j + 2) * YL, 128 * c : 128 * c + 128] = b
    for z in range(ZL):
        hs[z * YL : (z + 1) * YL, 256:384] = regroup([xi[b, 4] for b in range(PENCILS)], z)

    def end_step(j, c):
        at = pl.ds(pl.multiple_of(j * 160, 160), 160)
        h = jnp.concatenate([hs[at, 0:256], hs[at, 256:384][:, :64]], axis=1)
        vh, vl = split(h)
        out[at, :] = dm[at, :] + grid_mixing * dot3(vh, vl, tx0[...], tx1[...])
        return c

    lax.fori_loop(0, 4, end_step, 0)
    for finish in done:
        finish()


def body(
    density_history, residual_history, occupancy_history, occupancy_residual, species, slot_count
):
    mask = block_mask(species, slot_count)
    qx = real_basis(NX)
    qz = real_basis(NZ)
    qz = qz.reshape(NZ, SLABS, ZL).transpose(0, 2, 1).reshape(NZ, NZ)
    tables = two_parts(qx) + two_parts(qx.T) + two_parts(qz) + two_parts(qz.T)
    f32 = jnp.float32
    bf16 = jnp.bfloat16
    vmem = pl.BlockSpec(memory_space=pltpu.VMEM)
    hbm = pl.BlockSpec(memory_space=pl.ANY)
    rows = ZL * YL
    new_density, new_occupancy = pl.pallas_call(
        kernel,
        in_specs=[hbm, hbm, vmem, vmem, vmem] + [hbm] * 8,
        out_specs=[vmem, vmem],
        out_shape=[
            jax.ShapeDtypeStruct((rows, NX), f32),
            jax.ShapeDtypeStruct(mask.shape, f32),
        ],
        scratch_shapes=[
            pltpu.VMEM((H, rows, NX), f32),
            pltpu.VMEM((H, rows, NX), f32),
        ]
        + [pltpu.VMEM((NX, NX), bf16)] * 4
        + [pltpu.VMEM((NZ, NZ), bf16)] * 4
        + [
            pltpu.VMEM((1, 1, 128), f32),
            pltpu.VMEM((PENCILS, 1, 128), f32),
            pltpu.VMEM((1, 1, 128), f32),
            pltpu.VMEM((SLABS, 1, 128), f32),
            pltpu.VMEM((8, 128), f32),
            pltpu.VMEM((rows, NX), bf16),
            pltpu.VMEM((rows, NX), bf16),
            pltpu.VMEM((rows, 384), f32),
            pltpu.VMEM((PENCILS, LT, YL, 128), f32),
            pltpu.VMEM((PENCILS, LT, YL, 128), f32),
            pltpu.VMEM((LT, NY, 128), f32),
            pltpu.VMEM((LT, KY, SLABS, 128), f32),
            pltpu.VMEM((NZ, 512), bf16),
            pltpu.VMEM((NZ, 512), bf16),
            pltpu.VMEM((NZ, 512), f32),
            pltpu.VMEM((NZ, 512), f32),
            pltpu.VMEM((LT, KY, SLABS, 128), f32),
            pltpu.VMEM((LT, NY, 128), f32),
            pltpu.VMEM((PENCILS, LT, YL, 128), f32),
            pltpu.VMEM((PENCILS, LT, YL, 128), f32),
            pltpu.VMEM((rows, NX), f32),
            pltpu.SemaphoreType.DMA((ZL,)),
            pltpu.SemaphoreType.DMA((9,)),
            pltpu.SemaphoreType.DMA((6,)),
            pltpu.SemaphoreType.DMA((6,)),
        ],
        compiler_params=pltpu.CompilerParams(
            collective_id=0, has_side_effects=True, vmem_limit_bytes=56 * 2**20
        ),
    )(
        residual_history.reshape(H, rows, NX),
        density_history.reshape(H, rows, NX),
        occupancy_history,
        occupancy_residual,
        mask,
        *tables,
    )
    return (new_density.reshape(ZL, YL, NX), new_occupancy)


def solution(mesh):
    torus = Mesh(
        mesh.devices.reshape(8, 4, 2, mesh.shape["pencil"]),
        ("slab_0", "slab_1", "slab_2", "pencil"),
    )
    placed = (
        P(None, SLAB, "pencil", None),
        P(None, SLAB, "pencil", None),
        P(None, SLAB_PENCIL, None),
        P(None, SLAB_PENCIL, None),
        P(SLAB_PENCIL),
        P(SLAB_PENCIL),
    )
    return jax.shard_map(
        body,
        mesh=torus,
        in_specs=placed,
        out_specs=(P(SLAB, "pencil", None), P(SLAB_PENCIL, None)),
        check_vma=False,
    )
```

```python
import functools
import math

import numpy as np

import jax
import jax.numpy as jnp
from jax import lax
from jax.experimental import pallas as pl
from jax.experimental.pallas import tpu as pltpu
from jax.sharding import Mesh
from jax.sharding import PartitionSpec as P

ORBITALS = 18
SLAB = ("slab_0", "slab_1", "slab_2")
SLAB_PENCIL = ("slab_0", "slab_1", "slab_2", "pencil")
MESH = pl.DeviceIdType.MESH

grid_mixing = 0.5
block_mixing = 0.5
kerker_wave = 6.0
species_orbitals = (18, 13, 8, 5)

H = 7
SLABS = 64
PENCILS = 4
ZL = 8
YL = 80
NX = 320
NY = YL * PENCILS
NZ = ZL * SLABS
KY = NY // SLABS
LT = 5
CHUNKS = ((0,), (1, 2), (3, 4))
EIGHT = 8
PAIRS = [(i, j) for i in range(H) for j in range(i + 1)]


def real_basis(length):
    half = length // 2
    n = np.arange(length)
    rows = [np.full(length, 1.0 / math.sqrt(length))]
    for k in range(1, half):
        angle = 2.0 * math.pi * ((k * n) % length) / length
        rows.append(math.sqrt(2.0 / length) * np.cos(angle))
        rows.append(math.sqrt(2.0 / length) * np.sin(angle))
    rows.append(np.where(n % 2 == 0, 1.0, -1.0) / math.sqrt(length))
    return np.stack(rows)


def two_parts(table):
    upper = table.astype(np.float32).astype(jnp.bfloat16)
    lower = (table - upper.astype(np.float64)).astype(np.float32).astype(jnp.bfloat16)
    return upper, lower


def block_mask(species, slot_count):
    live = jnp.arange(species.shape[0], dtype=jnp.int32) < slot_count[0]
    orbitals = jnp.zeros_like(species)
    for species_index, orbital_number in enumerate(species_orbitals):
        orbitals = orbitals + orbital_number * (species == species_index).astype(jnp.int32)
    entry = jnp.arange(ORBITALS * ORBITALS, dtype=jnp.int32)
    row_index = entry // ORBITALS
    column_index = entry % ORBITALS
    inside = (
        (row_index[None, :] < orbitals[:, None])
        & (column_index[None, :] < orbitals[:, None])
        & live[:, None]
    )
    return inside.astype(jnp.float32)


def split(value):
    upper = value.astype(jnp.bfloat16)
    lower = (value - upper.astype(jnp.float32)).astype(jnp.bfloat16)
    return upper, lower


def dot3(ah, al, bh, bl):
    dot = functools.partial(jnp.dot, preferred_element_type=jnp.float32)
    return dot(ah, bh) + (dot(ah, bl) + dot(al, bh))


def lanes_of(shape):
    return lax.broadcasted_iota(jnp.int32, shape, 1)


def regroup(pieces, place):
    lane = lanes_of(pieces[0].shape)
    total = jnp.zeros_like(pieces[0])
    for n, piece in enumerate(pieces):
        moved = pltpu.roll(piece, lax.rem(16 * (n - place) + 128, 128), 1)
        total = jnp.where((lane >= 16 * n) & (lane < 16 * n + 16), moved, total)
    return total


def repeat(count, step):
    lax.fori_loop(0, count, lambda i, c: (step(i), c)[1], 0)


def kernel(
    res, den, occ_h, occ_r, mask, t0, t1, t2, t3, t4, t5, t6, t7,
    out, occ_out,
    r7, d7, tx0, tx1, tx2, tx3, tz0, tz1, tz2, tz3,
    row_mine, row_pencil, row_group, row_slab, weight,
    mh, ml, hs, xs, yin, ys, zin, zh, zl, fac, zu, zout, yb, yo, xi, dm,
    load_sem, table_sem, send_sem, recv_sem,
):
    s0, s1, s2 = (lax.axis_index(a) for a in SLAB)
    me_p = lax.axis_index("pencil")
    me_s = (s0 * 4 + s1) * 2 + s2

    def slab_each(act, cores=2):
        near = []
        for d in range(4 * cores):
            y, core = lax.rem(s1 + d // cores, 4), s2 if d % cores == 0 else 1 - s2
            near.append((y * cores + (core if cores == 2 else 0), y, core))

        def plane(z, some):
            for k, y, core in some:
                act(z * (4 * cores) + k, (z, y, core, me_p))

        plane(lax.rem(s0 + 4, 8), near)

        def pair(i):
            plane(lax.rem(s0 + 3 - i, 8), near)
            plane(lax.rem(s0 + 5 + i, 8), near)

        repeat(3, pair)
        plane(s0, near[1:])

    def pencil_each(act):
        for r in (2, 1, 3):
            q = lax.rem(me_p + r, PENCILS)
            act(q, (s0, s1, s2, q))

    me_e = s2 * PENCILS + me_p
    me_c = s0 * 4 + s1

    def eight_each(act):
        for r in range(1, EIGHT):
            q = lax.rem(me_p + r, PENCILS)
            core = s2 if r < PENCILS else 1 - s2
            act(core * PENCILS + q, (s0, s1, core, q))

    loads = []
    for z in range(ZL):
        rows = pl.ds(z * YL, YL)
        loads.append(pltpu.make_async_copy(res.at[:, rows], r7.at[:, rows], load_sem.at[z]))
    for c in loads:
        c.start()
    tables = []
    for n, (a, b) in enumerate(
        zip((t0, t1, t2, t3, t4, t5, t6, t7), (tx0, tx1, tx2, tx3, tz0, tz1, tz2, tz3))
    ):
        tables.append(pltpu.make_async_copy(a, b, table_sem.at[n]))
    tables.append(pltpu.make_async_copy(den, d7, table_sem.at[8]))

    barrier = pltpu.get_barrier_semaphore()
    def greet(q, device):
        pl.semaphore_signal(barrier, inc=1, device_id=device, device_id_type=MESH)

    eight_each(greet)
    slab_each(greet)

    zero = jnp.zeros((8, 128), jnp.float32)

    def add_products(acc, v):
        return [acc[n] + v[i] * v[j] for n, (i, j) in enumerate(PAIRS)]

    def pad(v):
        return jnp.concatenate([v, jnp.zeros((8, 128 - v.shape[1]), v.dtype)], axis=1)

    def block_step(r, acc):
        at = pl.ds(pl.multiple_of(r * 8, 8), 8)
        acc = list(acc)
        for lo, hi in ((0, 128), (128, 256), (256, 324)):
            m = mask[at, lo:hi]
            v = [occ_r[i, at, lo:hi] * m for i in range(H)]
            acc = add_products(acc, v if hi - lo == 128 else [pad(x) for x in v])
        return tuple(acc)

    block = lax.fori_loop(0, 3, block_step, (zero,) * len(PAIRS))
    cells = NX * NY * NZ
    scale = cells / (100.0 * SLABS * PENCILS * mask.shape[0])
    acc = tuple(x * scale for x in block)

    def grid_step(r, acc):
        at = pl.ds(pl.multiple_of(r * 8, 8), 8)
        acc = list(acc)
        for lo, hi in ((0, 128), (128, 256), (256, 320)):
            v = [r7[i, at, lo:hi] for i in range(H)]
            acc = add_products(acc, v if hi - lo == 128 else [pad(x) for x in v])
        return tuple(acc)

    for z in range(ZL):
        loads[z].wait()
        acc = lax.fori_loop(z * 10, z * 10 + 10, grid_step, acc)
    for c in tables:
        c.start()

    lane = lanes_of((8, 128))
    sub = lax.broadcasted_iota(jnp.int32, (8, 128), 0)
    spread = zero
    for n0 in range(0, len(PAIRS), 8):
        tile = zero
        for r, x in enumerate(acc[n0 : n0 + 8]):
            tile = jnp.where(sub == r, jnp.sum(x, axis=0, keepdims=True), tile)
        column = jnp.sum(tile, axis=1, keepdims=True)
        for r, (i, j) in enumerate(PAIRS[n0 : n0 + 8]):
            here = (sub == r) & ((lane == 8 * i + j) | (lane == 8 * j + i))
            spread = jnp.where(here, column, spread)
    row_mine[0] = jnp.sum(spread, axis=0, keepdims=True)

    pl.semaphore_wait(barrier, EIGHT - 1 + SLABS - 1)

    def exchange(phase, source_at, target, me, each, sent):
        def start(q, device):
            pltpu.make_async_remote_copy(
                src_ref=source_at(q),
                dst_ref=target(me),
                send_sem=send_sem.at[phase],
                recv_sem=recv_sem.at[phase],
                device_id=device,
                device_id_type=MESH,
            ).start()

        each(start)
        pltpu.make_async_copy(source_at(me), target(me), recv_sem.at[phase]).start()
        return pltpu.make_async_copy(sent, sent, send_sem.at[phase]).wait

    def arrive(phase, whole):
        pltpu.make_async_copy(whole, whole, recv_sem.at[phase]).wait()

    done = []
    done.append(
        exchange(
            0, lambda q: row_mine.at[0], lambda m: row_pencil.at[m], me_e, eight_each,
            row_pencil.at[pl.ds(0, EIGHT - 1)],
        )
    )
    arrive(0, row_pencil)
    group = row_pencil.reshape(EIGHT, 128)[...]
    row_group[0] = jnp.sum(group, axis=0, keepdims=True)
    done.append(
        exchange(
            1, lambda q: row_group.at[0], lambda m: row_slab.at[m], me_c,
            lambda act: slab_each(act, 1), row_slab.at[pl.ds(0, SLABS // 2 - 1)],
        )
    )

    def factor_step(r):
        at = pl.ds(pl.multiple_of(r * 8, 8), 8)
        kz = (lax.broadcasted_iota(jnp.int32, (8, 128), 0) + r * 8 + 1) // 2
        ky = (me_s * KY + lane // 16 + 1) // 2
        for g in range(LT):
            kx = (64 * g + 16 * me_p + lax.rem(lane, 16) + 1) // 2
            square = (kz * kz + ky * ky + kx * kx).astype(jnp.float32)
            fac[at, 128 * g : 128 * g + 128] = square / (square + kerker_wave * kerker_wave)

    repeat(NZ // 8, factor_step)

    arrive(1, row_slab)
    total = row_slab.reshape(SLABS // 2, 128)[...]
    total = jnp.sum(total, axis=0, keepdims=True) * (1.0 / cells)

    m = zero
    for i in range(H):
        m = jnp.where(sub == i, pltpu.roll(total, (128 - 8 * i) % 128, 1) if i else total, m)
    m = jnp.where(lane < H, m, 0.0)
    m = jnp.where((lane == H) & (sub < H), 1.0, m)
    for k in range(H):
        pivot_row = m[k : k + 1, :] / m[k : k + 1, k : k + 1]
        m = jnp.where(sub == k, pivot_row, m - m[:, k : k + 1] * pivot_row)
    solved = m[:, H : H + 1]
    weight[...] = jnp.broadcast_to(solved / jnp.sum(solved, axis=0, keepdims=True), (8, 128))

    w320 = [jnp.broadcast_to(weight[i : i + 1, 0:1], (16, NX)) for i in range(H)]

    def mix_step(r):
        at = pl.ds(pl.multiple_of(r * 16, 16), 16)
        v = w320[0] * r7[0, at]
        for i in range(1, H):
            v += w320[i] * r7[i, at]
        mh[at, :], ml[at, :] = split(v)

    repeat(ZL * YL // 16, mix_step)
    for c in tables[:4]:
        c.wait()

    def phase(c, stage):
        return 2 + 4 * c + stage

    for c, chunk in enumerate(CHUNKS):
        g0, g1 = chunk[0], chunk[-1] + 1
        n = g1 - g0
        tile = slice(128 * c, 128 * c + 128)

        def x_step(j):
            at = pl.ds(pl.multiple_of(j * 160, 160), 160)
            columns = slice(64 * g0, 64 * g1)
            h = dot3(mh[at, :], ml[at, :], tx2[:, columns], tx3[:, columns])
            if n == 1:
                h = jnp.concatenate([h, jnp.zeros((160, 64), jnp.float32)], axis=1)
            hs[at, tile] = h

        repeat(4, x_step)

        def x_pack(b):
            planes = [hs[z * YL : (z + 1) * YL, tile] for z in range(ZL)]
            for g in chunk:
                xs[b, g] = regroup(planes, 4 * (g - g0) + b)

        repeat(PENCILS, x_pack)
        done.append(
            exchange(
                phase(c, 0),
                lambda q, g0=g0, n=n: xs.at[q, pl.ds(g0, n)],
                lambda m, g0=g0, n=n: yin.at[m, pl.ds(g0, n)],
                me_p, pencil_each, xs.at[pl.ds(0, PENCILS - 1), pl.ds(g0, n)],
            )
        )

    for c in tables[4:]:
        c.wait()

    def density_step(r):
        at = pl.ds(pl.multiple_of(r * 16, 16), 16)
        v = w320[0] * d7[0, at]
        for i in range(1, H):
            v += w320[i] * d7[i, at]
        dm[at, :] = v

    ys_rows = ys.reshape(LT, NY, 1, 128)
    zin_rows = zin.reshape(LT, KY, SLABS, 1, 128)
    zout_rows = zout.reshape(LT, KY, SLABS, 1, 128)
    yb_rows = yb.reshape(LT, NY, 1, 128)
    for c, chunk in enumerate(CHUNKS):
        g0, n = chunk[0], len(chunk)
        arrive(phase(c, 0), yin.at[:, pl.ds(g0, n)])
        y = jnp.concatenate([yin[:, g].reshape(NY, 128) for g in chunk], axis=1)
        y = dot3(tx0[...], tx1[...], *split(y))
        for g in chunk:
            ys[g] = y[:, 128 * (g - g0) : 128 * (g - g0) + 128]
        done.append(
            exchange(
                phase(c, 1),
                lambda q, g0=g0, n=n: ys_rows.at[pl.ds(g0, n), pl.ds(q * KY, KY)],
                lambda m, g0=g0, n=n: zin_rows.at[pl.ds(g0, n), :, m],
                me_s, slab_each, ys_rows.at[pl.ds(g0, n), pl.ds(0, NY - KY)],
            )
        )

    repeat(ZL * YL // 16, density_step)
    for lo, hi in ((0, 128), (128, 256), (256, 324)):
        v = jnp.zeros((24, hi - lo), jnp.float32)
        for i in range(H):
            w = jnp.broadcast_to(weight[i : i + 1, 0:1], (24, hi - lo))
            v += w * (occ_h[i, :, lo:hi] + block_mixing * occ_r[i, :, lo:hi])
        occ_out[:, lo:hi] = mask[:, lo:hi] * v

    for c, chunk in enumerate(CHUNKS):
        g0, n = chunk[0], len(chunk)
        width = slice(0, 128 * n)
        arrive(phase(c, 1), zin.at[pl.ds(g0, n)])

        def z_pack(z):
            at = pl.ds(pl.multiple_of(z * 64, 64), 64)
            for g in chunk:
                lanes = slice(128 * (g - g0), 128 * (g - g0) + 128)
                zh[at, lanes], zl[at, lanes] = split(
                    regroup([zin[g, ky] for ky in range(KY)], z)
                )

        repeat(ZL, z_pack)
        zu[:, width] = dot3(tz0[...], tz1[...], zh[:, width], zl[:, width])

        def z_filter(z):
            at = pl.ds(pl.multiple_of(z * 64, 64), 64)
            v = zu[at, width] * fac[at, 128 * g0 : 128 * (g0 + n)]
            zh[at, width], zl[at, width] = split(v)

        repeat(ZL, z_filter)
        zu[:, width] = dot3(tz2[...], tz3[...], zh[:, width], zl[:, width])

        def z_unpack(ky):
            for g in chunk:
                lanes = slice(128 * (g - g0), 128 * (g - g0) + 128)
                planes = [zu[64 * z : 64 * z + 64, lanes] for z in range(ZL)]
                zout[g, ky] = regroup(planes, ky)

        repeat(KY, z_unpack)
        done.append(
            exchange(
                phase(c, 2),
                lambda q, g0=g0, n=n: zout_rows.at[pl.ds(g0, n), :, q],
                lambda m, g0=g0, n=n: yb_rows.at[pl.ds(g0, n), pl.ds(m * KY, KY)],
                me_s, slab_each, zout_rows.at[pl.ds(g0, n), :, pl.ds(0, SLABS - 1)],
            )
        )

    for c, chunk in enumerate(CHUNKS):
        g0, n = chunk[0], len(chunk)
        arrive(phase(c, 2), yb.at[pl.ds(g0, n)])
        y = jnp.concatenate([yb[g] for g in chunk], axis=1)
        y = dot3(tx2[...], tx3[...], *split(y))
        for g in chunk:
            lanes = slice(128 * (g - g0), 128 * (g - g0) + 128)
            yo[:, g] = y[:, lanes].reshape(PENCILS, YL, 128)
        done.append(
            exchange(
                phase(c, 3),
                lambda q, g0=g0, n=n: yo.at[q, pl.ds(g0, n)],
                lambda m, g0=g0, n=n: xi.at[m, pl.ds(g0, n)],
                me_p, pencil_each, yo.at[pl.ds(0, PENCILS - 1), pl.ds(g0, n)],
            )
        )

    for c, chunk in enumerate(CHUNKS):
        g0, g1 = chunk[0], chunk[-1] + 1
        n = g1 - g0
        tile = slice(128 * c, 128 * c + 64 * n)
        rows = slice(64 * g0, 64 * g1)
        arrive(phase(c, 3), xi.at[:, pl.ds(g0, n)])

        def end_step(z):
            at = pl.ds(pl.multiple_of(z * YL, YL), YL)
            h = regroup([xi[b, g] for g in chunk for b in range(PENCILS)], z)
            hh, hl = split(h[:, : 64 * n])
            v = dm[at, :] + grid_mixing * dot3(hh, hl, tx0[rows, :], tx1[rows, :])
            if c == len(CHUNKS) - 1:
                out[at, :] = v
            else:
                dm[at, :] = v

        repeat(ZL, end_step)
    for finish in done:
        finish()


def body(
    density_history, residual_history, occupancy_history, occupancy_residual, species, slot_count
):
    mask = block_mask(species, slot_count)
    qx = real_basis(NX)
    qz = real_basis(NZ)
    qz = qz.reshape(NZ, SLABS, ZL).transpose(0, 2, 1).reshape(NZ, NZ)
    tables = two_parts(qx) + two_parts(qx.T) + two_parts(qz) + two_parts(qz.T)
    f32 = jnp.float32
    bf16 = jnp.bfloat16
    vmem = pl.BlockSpec(memory_space=pltpu.VMEM)
    hbm = pl.BlockSpec(memory_space=pl.ANY)
    rows = ZL * YL
    new_density, new_occupancy = pl.pallas_call(
        kernel,
        in_specs=[hbm, hbm, vmem, vmem, vmem] + [hbm] * 8,
        out_specs=[vmem, vmem],
        out_shape=[
            jax.ShapeDtypeStruct((rows, NX), f32),
            jax.ShapeDtypeStruct(mask.shape, f32),
        ],
        scratch_shapes=[
            pltpu.VMEM((H, rows, NX), f32),
            pltpu.VMEM((H, rows, NX), f32),
        ]
        + [pltpu.VMEM((NX, NX), bf16)] * 4
        + [pltpu.VMEM((NZ, NZ), bf16)] * 4
        + [
            pltpu.VMEM((1, 1, 128), f32),
            pltpu.VMEM((EIGHT, 1, 128), f32),
            pltpu.VMEM((1, 1, 128), f32),
            pltpu.VMEM((SLABS // 2, 1, 128), f32),
            pltpu.VMEM((8, 128), f32),
            pltpu.VMEM((rows, NX), bf16),
            pltpu.VMEM((rows, NX), bf16),
            pltpu.VMEM((rows, 128 * len(CHUNKS)), f32),
            pltpu.VMEM((PENCILS, LT, YL, 128), f32),
            pltpu.VMEM((PENCILS, LT, YL, 128), f32),
            pltpu.VMEM((LT, NY, 128), f32),
            pltpu.VMEM((LT, KY, SLABS, 128), f32),
            pltpu.VMEM((NZ, 256), bf16),
            pltpu.VMEM((NZ, 256), bf16),
            pltpu.VMEM((NZ, 128 * LT), f32),
            pltpu.VMEM((NZ, 256), f32),
            pltpu.VMEM((LT, KY, SLABS, 128), f32),
            pltpu.VMEM((LT, NY, 128), f32),
            pltpu.VMEM((PENCILS, LT, YL, 128), f32),
            pltpu.VMEM((PENCILS, LT, YL, 128), f32),
            pltpu.VMEM((rows, NX), f32),
            pltpu.SemaphoreType.DMA((ZL,)),
            pltpu.SemaphoreType.DMA((9,)),
            pltpu.SemaphoreType.DMA((2 + 4 * len(CHUNKS),)),
            pltpu.SemaphoreType.DMA((2 + 4 * len(CHUNKS),)),
        ],
        compiler_params=pltpu.CompilerParams(
            collective_id=0, has_side_effects=True, vmem_limit_bytes=56 * 2**20
        ),
    )(
        residual_history.reshape(H, rows, NX),
        density_history.reshape(H, rows, NX),
        occupancy_history,
        occupancy_residual,
        mask,
        *tables,
    )
    return (new_density.reshape(ZL, YL, NX), new_occupancy)


def solution(mesh):
    torus = Mesh(
        mesh.devices.reshape(8, 4, 2, mesh.shape["pencil"]),
        ("slab_0", "slab_1", "slab_2", "pencil"),
    )
    placed = (
        P(None, SLAB, "pencil", None),
        P(None, SLAB, "pencil", None),
        P(None, SLAB_PENCIL, None),
        P(None, SLAB_PENCIL, None),
        P(SLAB_PENCIL),
        P(SLAB_PENCIL),
    )
    return jax.shard_map(
        body,
        mesh=torus,
        in_specs=placed,
        out_specs=(P(SLAB, "pencil", None), P(SLAB_PENCIL, None)),
        check_vma=False,
    )
```

```python
import functools
import math

import numpy as np

import jax
import jax.numpy as jnp
from jax import lax
from jax.experimental import pallas as pl
from jax.experimental.pallas import tpu as pltpu
from jax.sharding import Mesh
from jax.sharding import PartitionSpec as P

ORBITALS = 18
SLAB = ("slab_0", "slab_1", "slab_2")
SLAB_PENCIL = ("slab_0", "slab_1", "slab_2", "pencil")
MESH = pl.DeviceIdType.MESH

grid_mixing = 0.5
block_mixing = 0.5
kerker_wave = 6.0
species_orbitals = (18, 13, 8, 5)

H = 7
SLABS = 64
PENCILS = 4
ZL = 8
YL = 80
NX = 320
NY = YL * PENCILS
NZ = ZL * SLABS
KY = NY // SLABS
LT = 5
CHUNKS = ((0,), (1, 2), (3, 4))
EIGHT = 8
PAIRS = [(i, j) for i in range(H) for j in range(i + 1)]


def real_basis(length):
    half = length // 2
    n = np.arange(length)
    rows = [np.full(length, 1.0 / math.sqrt(length))]
    for k in range(1, half):
        angle = 2.0 * math.pi * ((k * n) % length) / length
        rows.append(math.sqrt(2.0 / length) * np.cos(angle))
        rows.append(math.sqrt(2.0 / length) * np.sin(angle))
    rows.append(np.where(n % 2 == 0, 1.0, -1.0) / math.sqrt(length))
    return np.stack(rows)


def two_parts(table):
    upper = table.astype(np.float32).astype(jnp.bfloat16)
    lower = (table - upper.astype(np.float64)).astype(np.float32).astype(jnp.bfloat16)
    return upper, lower


def split(value):
    upper = value.astype(jnp.bfloat16)
    lower = (value - upper.astype(jnp.float32)).astype(jnp.bfloat16)
    return upper, lower


def dot3(ah, al, bh, bl):
    dot = functools.partial(jnp.dot, preferred_element_type=jnp.float32)
    return dot(ah, bh) + (dot(ah, bl) + dot(al, bh))


def lanes_of(shape):
    return lax.broadcasted_iota(jnp.int32, shape, 1)


def regroup(pieces, place):
    lane = lanes_of(pieces[0].shape)
    total = jnp.zeros_like(pieces[0])
    for n, piece in enumerate(pieces):
        moved = pltpu.roll(piece, lax.rem(16 * (n - place) + 128, 128), 1)
        total = jnp.where((lane >= 16 * n) & (lane < 16 * n + 16), moved, total)
    return total


def repeat(count, step):
    lax.fori_loop(0, count, lambda i, c: (step(i), c)[1], 0)


def kernel(
    species, slot_count, res, den, occ_history, occ_residual, t0, t1, t2, t3, t4, t5, t6, t7,
    part_out, last_out, occ_out,
    occ_h, occ_r, mask,
    r7, d7, tx0, tx1, tx2, tx3, tz0, tz1, tz2, tz3,
    row_mine, row_pencil, row_group, row_slab, weight,
    mh, ml, hs, xs, yin, ys, zin, zh, zl, fac, zu, zout, yb, yo, xi, dm,
    load_sem, table_sem, send_sem, recv_sem,
):
    s0, s1, s2 = (lax.axis_index(a) for a in SLAB)
    me_p = lax.axis_index("pencil")
    me_s = (s0 * 4 + s1) * 2 + s2

    def slab_each(act, cores=2):
        near = []
        for d in range(4 * cores):
            y, core = lax.rem(s1 + d // cores, 4), s2 if d % cores == 0 else 1 - s2
            near.append((y * cores + (core if cores == 2 else 0), y, core))

        def plane(z, some):
            for k, y, core in some:
                act(z * (4 * cores) + k, (z, y, core, me_p))

        plane(lax.rem(s0 + 4, 8), near)

        def pair(i):
            plane(lax.rem(s0 + 3 - i, 8), near)
            plane(lax.rem(s0 + 5 + i, 8), near)

        repeat(3, pair)
        plane(s0, near[1:])

    def pencil_each(act):
        for r in (2, 1, 3):
            q = lax.rem(me_p + r, PENCILS)
            act(q, (s0, s1, s2, q))

    me_e = s2 * PENCILS + me_p
    me_c = s0 * 4 + s1

    def eight_each(act):
        for r in range(1, EIGHT):
            q = lax.rem(me_p + r, PENCILS)
            core = s2 if r < PENCILS else 1 - s2
            act(core * PENCILS + q, (s0, s1, core, q))

    loads = []
    for z in range(ZL):
        rows = pl.ds(z * YL, YL)
        loads.append(pltpu.make_async_copy(res.at[:, rows], r7.at[:, rows], load_sem.at[z]))
    for c in loads:
        c.start()
    tables = []
    for n, (a, b) in enumerate(
        zip((t0, t1, t2, t3, t4, t5, t6, t7), (tx0, tx1, tx2, tx3, tz0, tz1, tz2, tz3))
    ):
        tables.append(pltpu.make_async_copy(a, b, table_sem.at[n]))
    tables.append(pltpu.make_async_copy(den, d7, table_sem.at[8]))
    tables.append(pltpu.make_async_copy(occ_history, occ_h, table_sem.at[9]))
    occupancy = pltpu.make_async_copy(occ_residual, occ_r, load_sem.at[ZL])
    occupancy.start()

    barrier = pltpu.get_barrier_semaphore()
    def greet(q, device):
        pl.semaphore_signal(barrier, inc=1, device_id=device, device_id_type=MESH)

    eight_each(greet)
    slab_each(greet)

    zero = jnp.zeros((8, 128), jnp.float32)

    def add_products(acc, v):
        return [acc[n] + v[i] * v[j] for n, (i, j) in enumerate(PAIRS)]

    def pad(v):
        return jnp.concatenate([v, jnp.zeros((8, 128 - v.shape[1]), v.dtype)], axis=1)

    lane = lanes_of((8, 128))
    sub = lax.broadcasted_iota(jnp.int32, (8, 128), 0)
    for r0 in range(0, 24, 8):
        orbitals = jnp.zeros((8, 128), jnp.int32)
        for r in range(8):
            kind = species[r0 + r]
            number = jnp.int32(0)
            for index, value in enumerate(species_orbitals):
                number = jnp.where(kind == index, value, number)
            number = jnp.where(r0 + r < slot_count[0], number, 0)
            orbitals = jnp.where(sub == r, number, orbitals)
        for t in range(3):
            entry = lane + 128 * t
            column = entry
            for row in range(1, ORBITALS):
                column = jnp.where(entry >= ORBITALS * row, entry - ORBITALS * row, column)
            inside = (entry < ORBITALS * orbitals) & (column < orbitals)
            mask[r0 : r0 + 8, 128 * t : 128 * t + 128] = jnp.where(inside, 1.0, 0.0)

    def block_step(r, acc):
        at = pl.ds(pl.multiple_of(r * 8, 8), 8)
        acc = list(acc)
        for lo, hi in ((0, 128), (128, 256), (256, 324)):
            m = mask[at, lo:hi]
            v = [occ_r[i, at, lo:hi] * m for i in range(H)]
            acc = add_products(acc, v if hi - lo == 128 else [pad(x) for x in v])
        return tuple(acc)

    occupancy.wait()
    block = lax.fori_loop(0, 3, block_step, (zero,) * len(PAIRS))
    cells = NX * NY * NZ
    scale = cells / (100.0 * SLABS * PENCILS * mask.shape[0])
    acc = tuple(x * scale for x in block)

    def grid_step(r, acc):
        at = pl.ds(pl.multiple_of(r * 8, 8), 8)
        acc = list(acc)
        for lo, hi in ((0, 128), (128, 256), (256, 320)):
            v = [r7[i, at, lo:hi] for i in range(H)]
            acc = add_products(acc, v if hi - lo == 128 else [pad(x) for x in v])
        return tuple(acc)

    for z in range(ZL):
        loads[z].wait()
        acc = lax.fori_loop(z * 10, z * 10 + 10, grid_step, acc)
    for c in tables:
        c.start()

    spread = zero
    for n0 in range(0, len(PAIRS), 8):
        tile = zero
        for r, x in enumerate(acc[n0 : n0 + 8]):
            tile = jnp.where(sub == r, jnp.sum(x, axis=0, keepdims=True), tile)
        column = jnp.sum(tile, axis=1, keepdims=True)
        for r, (i, j) in enumerate(PAIRS[n0 : n0 + 8]):
            here = (sub == r) & ((lane == 8 * i + j) | (lane == 8 * j + i))
            spread = jnp.where(here, column, spread)
    row_mine[0] = jnp.sum(spread, axis=0, keepdims=True)

    pl.semaphore_wait(barrier, EIGHT - 1 + SLABS - 1)

    def exchange(phase, source_at, target, me, each, sent):
        def start(q, device):
            pltpu.make_async_remote_copy(
                src_ref=source_at(q),
                dst_ref=target(me),
                send_sem=send_sem.at[phase],
                recv_sem=recv_sem.at[phase],
                device_id=device,
                device_id_type=MESH,
            ).start()

        each(start)
        pltpu.make_async_copy(source_at(me), target(me), recv_sem.at[phase]).start()
        return pltpu.make_async_copy(sent, sent, send_sem.at[phase]).wait

    def arrive(phase, whole):
        pltpu.make_async_copy(whole, whole, recv_sem.at[phase]).wait()

    done = []
    done.append(
        exchange(
            0, lambda q: row_mine.at[0], lambda m: row_pencil.at[m], me_e, eight_each,
            row_pencil.at[pl.ds(0, EIGHT - 1)],
        )
    )
    arrive(0, row_pencil)
    group = row_pencil.reshape(EIGHT, 128)[...]
    row_group[0] = jnp.sum(group, axis=0, keepdims=True)
    done.append(
        exchange(
            1, lambda q: row_group.at[0], lambda m: row_slab.at[m], me_c,
            lambda act: slab_each(act, 1), row_slab.at[pl.ds(0, SLABS // 2 - 1)],
        )
    )

    def factor_step(r):
        at = pl.ds(pl.multiple_of(r * 8, 8), 8)
        kz = (lax.broadcasted_iota(jnp.int32, (8, 128), 0) + r * 8 + 1) // 2
        ky = (me_s * KY + lane // 16 + 1) // 2
        for g in range(LT):
            kx = (64 * g + 16 * me_p + lax.rem(lane, 16) + 1) // 2
            square = (kz * kz + ky * ky + kx * kx).astype(jnp.float32)
            fac[at, 128 * g : 128 * g + 128] = square / (square + kerker_wave * kerker_wave)

    repeat(NZ // 8, factor_step)

    arrive(1, row_slab)
    total = row_slab.reshape(SLABS // 2, 128)[...]
    total = jnp.sum(total, axis=0, keepdims=True) * (1.0 / cells)

    m = zero
    for i in range(H):
        m = jnp.where(sub == i, pltpu.roll(total, (128 - 8 * i) % 128, 1) if i else total, m)
    m = jnp.where(lane < H, m, 0.0)
    m = jnp.where((lane == H) & (sub < H), 1.0, m)
    for k in range(H):
        pivot_row = m[k : k + 1, :] / m[k : k + 1, k : k + 1]
        m = jnp.where(sub == k, pivot_row, m - m[:, k : k + 1] * pivot_row)
    solved = m[:, H : H + 1]
    weight[...] = jnp.broadcast_to(solved / jnp.sum(solved, axis=0, keepdims=True), (8, 128))

    w320 = [jnp.broadcast_to(weight[i : i + 1, 0:1], (16, NX)) for i in range(H)]

    def mix_step(r):
        at = pl.ds(pl.multiple_of(r * 16, 16), 16)
        v = w320[0] * r7[0, at]
        for i in range(1, H):
            v += w320[i] * r7[i, at]
        mh[at, :], ml[at, :] = split(v)

    repeat(ZL * YL // 16, mix_step)
    for c in tables[:4]:
        c.wait()

    def phase(c, stage):
        return 2 + 4 * c + stage

    for c, chunk in enumerate(CHUNKS):
        g0, g1 = chunk[0], chunk[-1] + 1
        n = g1 - g0
        tile = slice(128 * c, 128 * c + 128)

        def x_step(j):
            at = pl.ds(pl.multiple_of(j * 160, 160), 160)
            columns = slice(64 * g0, 64 * g1)
            h = dot3(mh[at, :], ml[at, :], tx2[:, columns], tx3[:, columns])
            if n == 1:
                h = jnp.concatenate([h, jnp.zeros((160, 64), jnp.float32)], axis=1)
            hs[at, tile] = h

        repeat(4, x_step)

        def x_pack(b):
            planes = [hs[z * YL : (z + 1) * YL, tile] for z in range(ZL)]
            for g in chunk:
                xs[b, g] = regroup(planes, 4 * (g - g0) + b)

        repeat(PENCILS, x_pack)
        done.append(
            exchange(
                phase(c, 0),
                lambda q, g0=g0, n=n: xs.at[q, pl.ds(g0, n)],
                lambda m, g0=g0, n=n: yin.at[m, pl.ds(g0, n)],
                me_p, pencil_each, xs.at[pl.ds(0, PENCILS - 1), pl.ds(g0, n)],
            )
        )

    for c in tables[4:]:
        c.wait()

    def density_step(r):
        at = pl.ds(pl.multiple_of(r * 16, 16), 16)
        v = w320[0] * d7[0, at]
        for i in range(1, H):
            v += w320[i] * d7[i, at]
        dm[at, :] = v

    ys_rows, zin_rows, zout_rows, yb_rows = (
        ref.reshape(LT * NY, 1, 128) for ref in (ys, zin, zout, yb)
    )
    for c, chunk in enumerate(CHUNKS):
        g0, n = chunk[0], len(chunk)
        arrive(phase(c, 0), yin.at[:, pl.ds(g0, n)])
        y = jnp.concatenate([yin[:, g].reshape(NY, 128) for g in chunk], axis=1)
        y = dot3(tx0[...], tx1[...], *split(y))
        for g in range(n):
            ys[pl.ds(g0 * NY + g, NY, stride=n), :] = y[:, 128 * g : 128 * g + 128]
        done.append(
            exchange(
                phase(c, 1),
                lambda q, g0=g0, n=n: ys_rows.at[pl.ds(g0 * NY + q * (KY * n), KY * n)],
                lambda m, g0=g0, n=n: zin_rows.at[pl.ds(g0 * NY + m * (KY * n), KY * n)],
                me_s, slab_each, ys_rows.at[pl.ds(g0 * NY, (NY - KY) * n)],
            )
        )

    repeat(ZL * YL // 16, density_step)
    for lo, hi in ((0, 128), (128, 256), (256, 324)):
        v = jnp.zeros((24, hi - lo), jnp.float32)
        for i in range(H):
            w = jnp.broadcast_to(weight[i : i + 1, 0:1], (24, hi - lo))
            v += w * (occ_h[i, :, lo:hi] + block_mixing * occ_r[i, :, lo:hi])
        occ_out[:, lo:hi] = mask[:, lo:hi] * v

    for c, chunk in enumerate(CHUNKS):
        g0, n = chunk[0], len(chunk)
        width = slice(0, 128 * n)
        arrive(phase(c, 1), zin.at[pl.ds(g0 * NY, n * NY)])

        def z_pack(z):
            at = pl.ds(pl.multiple_of(z * 64, 64), 64)
            for g in range(n):
                lanes = slice(128 * g, 128 * g + 128)
                lines = [
                    zin[pl.ds(g0 * NY + ky * n + g, SLABS, stride=KY * n), :] for ky in range(KY)
                ]
                zh[at, lanes], zl[at, lanes] = split(regroup(lines, z))

        repeat(ZL, z_pack)
        zu[:, width] = dot3(tz0[...], tz1[...], zh[:, width], zl[:, width])

        def z_filter(z):
            at = pl.ds(pl.multiple_of(z * 64, 64), 64)
            v = zu[at, width] * fac[at, 128 * g0 : 128 * (g0 + n)]
            zh[at, width], zl[at, width] = split(v)

        repeat(ZL, z_filter)
        zu[:, width] = dot3(tz2[...], tz3[...], zh[:, width], zl[:, width])

        def z_unpack(ky):
            for g in range(n):
                lanes = slice(128 * g, 128 * g + 128)
                planes = [zu[64 * z : 64 * z + 64, lanes] for z in range(ZL)]
                at = pl.ds(g0 * NY + ky * n + g, SLABS, stride=KY * n)
                zout[at, :] = regroup(planes, ky)

        repeat(KY, z_unpack)
        done.append(
            exchange(
                phase(c, 2),
                lambda q, g0=g0, n=n: zout_rows.at[pl.ds(g0 * NY + q * (KY * n), KY * n)],
                lambda m, g0=g0, n=n: yb_rows.at[pl.ds(g0 * NY + m * (KY * n), KY * n)],
                me_s, slab_each, zout_rows.at[pl.ds(g0 * NY, (NY - KY) * n)],
            )
        )

    for c, chunk in enumerate(CHUNKS):
        g0, n = chunk[0], len(chunk)
        arrive(phase(c, 2), yb.at[pl.ds(g0 * NY, n * NY)])
        y = [yb[pl.ds(g0 * NY + g, NY, stride=n), :] for g in range(n)]
        y = jnp.concatenate(y, axis=1)
        y = dot3(tx2[...], tx3[...], *split(y))
        for g in chunk:
            lanes = slice(128 * (g - g0), 128 * (g - g0) + 128)
            yo[:, g] = y[:, lanes].reshape(PENCILS, YL, 128)
        done.append(
            exchange(
                phase(c, 3),
                lambda q, g0=g0, n=n: yo.at[q, pl.ds(g0, n)],
                lambda m, g0=g0, n=n: xi.at[m, pl.ds(g0, n)],
                me_p, pencil_each, yo.at[pl.ds(0, PENCILS - 1), pl.ds(g0, n)],
            )
        )

    for c, chunk in enumerate(CHUNKS):
        g0, g1 = chunk[0], chunk[-1] + 1
        n = g1 - g0
        rows = slice(64 * g0, 64 * g1)
        arrive(phase(c, 3), xi.at[:, pl.ds(g0, n)])
        if c == len(CHUNKS) - 1:
            break

        def end_step(z):
            at = pl.ds(pl.multiple_of(z * YL, YL), YL)
            h = regroup([xi[b, g] for g in chunk for b in range(PENCILS)], z)
            hh, hl = split(h[:, : 64 * n])
            dm[at, :] += grid_mixing * dot3(hh, hl, tx0[rows, :], tx1[rows, :])

        repeat(ZL, end_step)
        if c == len(CHUNKS) - 2:
            part = pltpu.make_async_copy(dm, part_out, load_sem.at[ZL + 1])
            part.start()
    last = pltpu.make_async_copy(xi.at[:, pl.ds(g0, n)], last_out, load_sem.at[ZL + 2])
    last.start()
    for finish in done:
        finish()
    part.wait()
    last.wait()


def last_kernel(part, last, tx0, tx1, occ, out, occ_out):
    n = last.shape[1]
    for half in range(2):
        at = slice(half * YL, half * YL + YL)
        z = 2 * pl.program_id(0) + half
        h = regroup([last[b, g] for g in range(n) for b in range(PENCILS)], z)
        rows = slice(NX - 64 * n, NX)
        hh, hl = split(h[:, : 64 * n])
        out[at, :] = part[at, :] + grid_mixing * dot3(hh, hl, tx0[rows, :], tx1[rows, :])

    @pl.when(pl.program_id(0) == 0)
    def _():
        occ_out[...] = occ[...]


def body(
    density_history, residual_history, occupancy_history, occupancy_residual, species, slot_count
):
    qx = real_basis(NX)
    qz = real_basis(NZ)
    qz = qz.reshape(NZ, SLABS, ZL).transpose(0, 2, 1).reshape(NZ, NZ)
    tables = two_parts(qx) + two_parts(qx.T) + two_parts(qz) + two_parts(qz.T)
    f32 = jnp.float32
    bf16 = jnp.bfloat16
    vmem = pl.BlockSpec(memory_space=pltpu.VMEM)
    hbm = pl.BlockSpec(memory_space=pl.ANY)
    smem = pl.BlockSpec(memory_space=pltpu.SMEM)
    slots, entries = occupancy_history.shape[1:]
    rows = ZL * YL
    last_tiles = len(CHUNKS[-1])
    part, last, occupancy = pl.pallas_call(
        kernel,
        in_specs=[smem, smem] + [hbm] * 12,
        out_specs=[hbm, hbm, vmem],
        out_shape=[
            jax.ShapeDtypeStruct((rows, NX), f32),
            jax.ShapeDtypeStruct((PENCILS, last_tiles, YL, 128), f32),
            jax.ShapeDtypeStruct((slots, entries), f32),
        ],
        scratch_shapes=[
            pltpu.VMEM((H, slots, entries), f32),
            pltpu.VMEM((H, slots, entries), f32),
            pltpu.VMEM((slots, 384), f32),
            pltpu.VMEM((H, rows, NX), f32),
            pltpu.VMEM((H, rows, NX), f32),
        ]
        + [pltpu.VMEM((NX, NX), bf16)] * 4
        + [pltpu.VMEM((NZ, NZ), bf16)] * 4
        + [
            pltpu.VMEM((1, 1, 128), f32),
            pltpu.VMEM((EIGHT, 1, 128), f32),
            pltpu.VMEM((1, 1, 128), f32),
            pltpu.VMEM((SLABS // 2, 1, 128), f32),
            pltpu.VMEM((8, 128), f32),
            pltpu.VMEM((rows, NX), bf16),
            pltpu.VMEM((rows, NX), bf16),
            pltpu.VMEM((rows, 128 * len(CHUNKS)), f32),
            pltpu.VMEM((PENCILS, LT, YL, 128), f32),
            pltpu.VMEM((PENCILS, LT, YL, 128), f32),
            pltpu.VMEM((LT * NY, 128), f32),
            pltpu.VMEM((LT * NY, 128), f32),
            pltpu.VMEM((NZ, 256), bf16),
            pltpu.VMEM((NZ, 256), bf16),
            pltpu.VMEM((NZ, 128 * LT), f32),
            pltpu.VMEM((NZ, 256), f32),
            pltpu.VMEM((LT * NY, 128), f32),
            pltpu.VMEM((LT * NY, 128), f32),
            pltpu.VMEM((PENCILS, LT, YL, 128), f32),
            pltpu.VMEM((PENCILS, LT, YL, 128), f32),
            pltpu.VMEM((rows, NX), f32),
            pltpu.SemaphoreType.DMA((ZL + 3,)),
            pltpu.SemaphoreType.DMA((10,)),
            pltpu.SemaphoreType.DMA((2 + 4 * len(CHUNKS),)),
            pltpu.SemaphoreType.DMA((2 + 4 * len(CHUNKS),)),
        ],
        compiler_params=pltpu.CompilerParams(
            collective_id=0, has_side_effects=True, vmem_limit_bytes=56 * 2**20
        ),
    )(
        species,
        slot_count,
        residual_history.reshape(H, rows, NX),
        density_history.reshape(H, rows, NX),
        occupancy_history,
        occupancy_residual,
        *tables,
    )
    new_density, new_occupancy = pl.pallas_call(
        last_kernel,
        grid=(ZL // 2,),
        in_specs=[
            pl.BlockSpec((2 * YL, NX), lambda z: (z, 0)),
            pl.BlockSpec(last.shape, lambda z: (0, 0, 0, 0)),
            pl.BlockSpec((NX, NX), lambda z: (0, 0)),
            pl.BlockSpec((NX, NX), lambda z: (0, 0)),
            pl.BlockSpec((slots, entries), lambda z: (0, 0)),
        ],
        out_specs=[
            pl.BlockSpec((2 * YL, NX), lambda z: (z, 0)),
            pl.BlockSpec((slots, entries), lambda z: (0, 0)),
        ],
        out_shape=[
            jax.ShapeDtypeStruct((rows, NX), f32),
            jax.ShapeDtypeStruct((slots, entries), f32),
        ],
    )(part, last, tables[0], tables[1], occupancy)
    return (new_density.reshape(ZL, YL, NX), new_occupancy)


def solution(mesh):
    torus = Mesh(
        mesh.devices.reshape(8, 4, 2, mesh.shape["pencil"]),
        ("slab_0", "slab_1", "slab_2", "pencil"),
    )
    placed = (
        P(None, SLAB, "pencil", None),
        P(None, SLAB, "pencil", None),
        P(None, SLAB_PENCIL, None),
        P(None, SLAB_PENCIL, None),
        P(SLAB_PENCIL),
        P(SLAB_PENCIL),
    )
    return jax.shard_map(
        body,
        mesh=torus,
        in_specs=placed,
        out_specs=(P(SLAB, "pencil", None), P(SLAB_PENCIL, None)),
        check_vma=False,
    )
```

```python
import functools
import math

import numpy as np

import jax
import jax.numpy as jnp
from jax import lax
from jax.experimental import pallas as pl
from jax.experimental.pallas import tpu as pltpu
from jax.sharding import Mesh
from jax.sharding import PartitionSpec as P

ORBITALS = 18
SLAB = ("slab_0", "slab_1", "slab_2")
SLAB_PENCIL = ("slab_0", "slab_1", "slab_2", "pencil")
MESH = pl.DeviceIdType.MESH

grid_mixing = 0.5
block_mixing = 0.5
kerker_wave = 6.0
species_orbitals = (18, 13, 8, 5)

H = 7
SLABS = 64
PENCILS = 4
ZL = 8
YL = 80
NX = 320
NY = YL * PENCILS
NZ = ZL * SLABS
KY = NY // SLABS
LT = 5
CHUNKS = ((0,), (1, 2), (3, 4))
EIGHT = 8
PAIRS = [(i, j) for i in range(H) for j in range(i + 1)]


def real_basis(length):
    half = length // 2
    n = np.arange(length)
    rows = [np.full(length, 1.0 / math.sqrt(length))]
    for k in range(1, half):
        angle = 2.0 * math.pi * ((k * n) % length) / length
        rows.append(math.sqrt(2.0 / length) * np.cos(angle))
        rows.append(math.sqrt(2.0 / length) * np.sin(angle))
    rows.append(np.where(n % 2 == 0, 1.0, -1.0) / math.sqrt(length))
    return np.stack(rows)


def two_parts(table):
    upper = table.astype(np.float32).astype(jnp.bfloat16)
    lower = (table - upper.astype(np.float64)).astype(np.float32).astype(jnp.bfloat16)
    return upper, lower


def split(value):
    upper = value.astype(jnp.bfloat16)
    lower = (value - upper.astype(jnp.float32)).astype(jnp.bfloat16)
    return upper, lower


def dot3(ah, al, bh, bl):
    dot = functools.partial(jnp.dot, preferred_element_type=jnp.float32)
    return dot(ah, bh) + (dot(ah, bl) + dot(al, bh))


def lanes_of(shape):
    return lax.broadcasted_iota(jnp.int32, shape, 1)


def regroup(pieces, place):
    lane = lanes_of(pieces[0].shape)
    total = jnp.zeros_like(pieces[0])
    for n, piece in enumerate(pieces):
        moved = pltpu.roll(piece, lax.rem(16 * (n - place) + 128, 128), 1)
        total = jnp.where((lane >= 16 * n) & (lane < 16 * n + 16), moved, total)
    return total


def repeat(count, step):
    lax.fori_loop(0, count, lambda i, c: (step(i), c)[1], 0)


def kernel(
    species, slot_count, res, den, occ_history, occ_residual, t0, t1, t2, t3, t4, t5, t6, t7,
    part_out, last_out, occ_out,
    occ_h, occ_r, mask,
    r7, d7, tx0, tx1, tx2, tx3, tz0, tz1, tz2, tz3,
    row_mine, row_pencil, row_group, row_slab, weight,
    mh, ml, hs, xs, yin, ys, zin, zh, zl, fac, zu, zout, yb, yo, xi, dm,
    load_sem, table_sem, send_sem, recv_sem,
):
    s0, s1, s2 = (lax.axis_index(a) for a in SLAB)
    me_p = lax.axis_index("pencil")
    me_s = (s0 * 4 + s1) * 2 + s2

    def slab_each(act, cores=2):
        near = []
        for d in range(4 * cores):
            y, core = lax.rem(s1 + d // cores, 4), s2 if d % cores == 0 else 1 - s2
            near.append((y * cores + (core if cores == 2 else 0), y, core))

        def plane(z, some):
            for k, y, core in some:
                act(z * (4 * cores) + k, (z, y, core, me_p))

        plane(lax.rem(s0 + 4, 8), near)

        def pair(i):
            plane(lax.rem(s0 + 3 - i, 8), near)
            plane(lax.rem(s0 + 5 + i, 8), near)

        repeat(3, pair)
        plane(s0, near[1:])

    def pencil_each(act):
        for r in (2, 1, 3):
            q = lax.rem(me_p + r, PENCILS)
            act(q, (s0, s1, s2, q))

    me_e = s2 * PENCILS + me_p
    me_c = s0 * 4 + s1

    def eight_each(act):
        for r in range(1, EIGHT):
            q = lax.rem(me_p + r, PENCILS)
            core = s2 if r < PENCILS else 1 - s2
            act(core * PENCILS + q, (s0, s1, core, q))

    loads = []
    for z in range(ZL):
        rows = pl.ds(z * YL, YL)
        loads.append(pltpu.make_async_copy(res.at[:, rows], r7.at[:, rows], load_sem.at[z]))
    for c in loads:
        c.start()
    tables = []
    for n, (a, b) in enumerate(
        zip((t0, t1, t2, t3, t4, t5, t6, t7), (tx0, tx1, tx2, tx3, tz0, tz1, tz2, tz3))
    ):
        tables.append(pltpu.make_async_copy(a, b, table_sem.at[n]))
    tables.append(pltpu.make_async_copy(den, d7, table_sem.at[8]))
    tables.append(pltpu.make_async_copy(occ_history, occ_h, table_sem.at[9]))
    occupancy = pltpu.make_async_copy(occ_residual, occ_r, load_sem.at[ZL])
    occupancy.start()

    barrier = pltpu.get_barrier_semaphore()
    def greet(q, device):
        pl.semaphore_signal(barrier, inc=1, device_id=device, device_id_type=MESH)

    eight_each(greet)
    slab_each(greet)

    zero = jnp.zeros((8, 128), jnp.float32)

    def add_products(acc, v):
        return [acc[n] + v[i] * v[j] for n, (i, j) in enumerate(PAIRS)]

    def pad(v):
        return jnp.concatenate([v, jnp.zeros((8, 128 - v.shape[1]), v.dtype)], axis=1)

    lane = lanes_of((8, 128))
    sub = lax.broadcasted_iota(jnp.int32, (8, 128), 0)
    for r0 in range(0, 24, 8):
        orbitals = jnp.zeros((8, 128), jnp.int32)
        for r in range(8):
            kind = species[r0 + r]
            number = jnp.int32(0)
            for index, value in enumerate(species_orbitals):
                number = jnp.where(kind == index, value, number)
            number = jnp.where(r0 + r < slot_count[0], number, 0)
            orbitals = jnp.where(sub == r, number, orbitals)
        for t in range(3):
            entry = lane + 128 * t
            column = entry
            for row in range(1, ORBITALS):
                column = jnp.where(entry >= ORBITALS * row, entry - ORBITALS * row, column)
            inside = (entry < ORBITALS * orbitals) & (column < orbitals)
            mask[r0 : r0 + 8, 128 * t : 128 * t + 128] = jnp.where(inside, 1.0, 0.0)

    def block_step(r, acc):
        at = pl.ds(pl.multiple_of(r * 8, 8), 8)
        acc = list(acc)
        for lo, hi in ((0, 128), (128, 256), (256, 324)):
            m = mask[at, lo:hi]
            v = [occ_r[i, at, lo:hi] * m for i in range(H)]
            acc = add_products(acc, v if hi - lo == 128 else [pad(x) for x in v])
        return tuple(acc)

    occupancy.wait()
    block = lax.fori_loop(0, 3, block_step, (zero,) * len(PAIRS))
    cells = NX * NY * NZ
    scale = cells / (100.0 * SLABS * PENCILS * mask.shape[0])
    acc = tuple(x * scale for x in block)

    def grid_step(r, acc):
        at = pl.ds(pl.multiple_of(r * 8, 8), 8)
        acc = list(acc)
        for lo, hi in ((0, 128), (128, 256), (256, 320)):
            v = [r7[i, at, lo:hi] for i in range(H)]
            acc = add_products(acc, v if hi - lo == 128 else [pad(x) for x in v])
        return tuple(acc)

    for z in range(ZL):
        loads[z].wait()
        acc = lax.fori_loop(z * 10, z * 10 + 10, grid_step, acc)
    for c in tables:
        c.start()

    spread = zero
    for n0 in range(0, len(PAIRS), 8):
        tile = zero
        for r, x in enumerate(acc[n0 : n0 + 8]):
            tile = jnp.where(sub == r, jnp.sum(x, axis=0, keepdims=True), tile)
        column = jnp.sum(tile, axis=1, keepdims=True)
        for r, (i, j) in enumerate(PAIRS[n0 : n0 + 8]):
            here = (sub == r) & ((lane == 8 * i + j) | (lane == 8 * j + i))
            spread = jnp.where(here, column, spread)
    row_mine[0] = jnp.sum(spread, axis=0, keepdims=True)

    pl.semaphore_wait(barrier, EIGHT - 1 + SLABS - 1)

    def exchange(phase, source_at, target, me, each, sent):
        def start(q, device):
            pltpu.make_async_remote_copy(
                src_ref=source_at(q),
                dst_ref=target(me),
                send_sem=send_sem.at[phase],
                recv_sem=recv_sem.at[phase],
                device_id=device,
                device_id_type=MESH,
            ).start()

        each(start)
        pltpu.make_async_copy(source_at(me), target(me), recv_sem.at[phase]).start()
        return pltpu.make_async_copy(sent, sent, send_sem.at[phase]).wait

    def arrive(phase, whole):
        pltpu.make_async_copy(whole, whole, recv_sem.at[phase]).wait()

    done = []
    done.append(
        exchange(
            0, lambda q: row_mine.at[0], lambda m: row_pencil.at[m], me_e, eight_each,
            row_pencil.at[pl.ds(0, EIGHT - 1)],
        )
    )
    arrive(0, row_pencil)
    group = row_pencil.reshape(EIGHT, 128)[...]
    row_group[0] = jnp.sum(group, axis=0, keepdims=True)
    done.append(
        exchange(
            1, lambda q: row_group.at[0], lambda m: row_slab.at[m], me_c,
            lambda act: slab_each(act, 1), row_slab.at[pl.ds(0, SLABS // 2 - 1)],
        )
    )

    def factor_step(r):
        at = pl.ds(pl.multiple_of(r * 8, 8), 8)
        kz = (lax.broadcasted_iota(jnp.int32, (8, 128), 0) + r * 8 + 1) // 2
        ky = (me_s * KY + lane // 16 + 1) // 2
        for g in range(LT):
            kx = (64 * g + 16 * me_p + lax.rem(lane, 16) + 1) // 2
            square = (kz * kz + ky * ky + kx * kx).astype(jnp.float32)
            fac[at, 128 * g : 128 * g + 128] = square / (square + kerker_wave * kerker_wave)

    repeat(NZ // 8, factor_step)

    arrive(1, row_slab)
    total = row_slab.reshape(SLABS // 2, 128)[...]
    total = jnp.sum(total, axis=0, keepdims=True) * (1.0 / cells)

    m = zero
    for i in range(H):
        m = jnp.where(sub == i, pltpu.roll(total, (128 - 8 * i) % 128, 1) if i else total, m)
    m = jnp.where(lane < H, m, 0.0)
    m = jnp.where((lane == H) & (sub < H), 1.0, m)
    for k in range(H):
        pivot_row = m[k : k + 1, :] / m[k : k + 1, k : k + 1]
        m = jnp.where(sub == k, pivot_row, m - m[:, k : k + 1] * pivot_row)
    solved = m[:, H : H + 1]
    weight[...] = jnp.broadcast_to(solved / jnp.sum(solved, axis=0, keepdims=True), (8, 128))

    w320 = [jnp.broadcast_to(weight[i : i + 1, 0:1], (16, NX)) for i in range(H)]

    def mix_step(r):
        at = pl.ds(pl.multiple_of(r * 16, 16), 16)
        v = w320[0] * r7[0, at]
        for i in range(1, H):
            v += w320[i] * r7[i, at]
        mh[at, :], ml[at, :] = split(v)

    repeat(ZL * YL // 16, mix_step)
    for c in tables[:4]:
        c.wait()

    def phase(c, stage):
        return 2 + 4 * c + stage

    for c, chunk in enumerate(CHUNKS):
        g0, g1 = chunk[0], chunk[-1] + 1
        n = g1 - g0
        tile = slice(128 * c, 128 * c + 128)

        def x_step(j):
            at = pl.ds(pl.multiple_of(j * 160, 160), 160)
            columns = slice(64 * g0, 64 * g1)
            h = dot3(mh[at, :], ml[at, :], tx2[:, columns], tx3[:, columns])
            if n == 1:
                h = jnp.concatenate([h, jnp.zeros((160, 64), jnp.float32)], axis=1)
            hs[at, tile] = h

        repeat(4, x_step)

        def x_pack(b):
            planes = [hs[z * YL : (z + 1) * YL, tile] for z in range(ZL)]
            for g in chunk:
                xs[b, g] = regroup(planes, 4 * (g - g0) + b)

        def pack_each(act):
            ready = None
            for r in (2, 1, 3, 0):
                q = lax.rem(me_p + r, PENCILS)
                x_pack(q)
                if ready is not None:
                    act(*ready)
                ready = (q, (s0, s1, s2, q))

        if c > 0:
            repeat(PENCILS, x_pack)
        done.append(
            exchange(
                phase(c, 0),
                lambda q, g0=g0, n=n: xs.at[q, pl.ds(g0, n)],
                lambda m, g0=g0, n=n: yin.at[m, pl.ds(g0, n)],
                me_p, pencil_each if c > 0 else pack_each,
                xs.at[pl.ds(0, PENCILS - 1), pl.ds(g0, n)],
            )
        )

    for c in tables[4:]:
        c.wait()

    def density_step(r):
        at = pl.ds(pl.multiple_of(r * 16, 16), 16)
        v = w320[0] * d7[0, at]
        for i in range(1, H):
            v += w320[i] * d7[i, at]
        dm[at, :] = v

    ys_rows, zin_rows, zout_rows, yb_rows = (
        ref.reshape(LT * NY, 1, 128) for ref in (ys, zin, zout, yb)
    )
    for c, chunk in enumerate(CHUNKS):
        g0, n = chunk[0], len(chunk)
        arrive(phase(c, 0), yin.at[:, pl.ds(g0, n)])
        y = jnp.concatenate([yin[:, g].reshape(NY, 128) for g in chunk], axis=1)
        y = dot3(tx0[...], tx1[...], *split(y))
        for g in range(n):
            ys[pl.ds(g0 * NY + g, NY, stride=n), :] = y[:, 128 * g : 128 * g + 128]
        done.append(
            exchange(
                phase(c, 1),
                lambda q, g0=g0, n=n: ys_rows.at[pl.ds(g0 * NY + q * (KY * n), KY * n)],
                lambda m, g0=g0, n=n: zin_rows.at[pl.ds(g0 * NY + m * (KY * n), KY * n)],
                me_s, slab_each, ys_rows.at[pl.ds(g0 * NY, (NY - KY) * n)],
            )
        )

    repeat(ZL * YL // 16, density_step)
    for lo, hi in ((0, 128), (128, 256), (256, 324)):
        v = jnp.zeros((24, hi - lo), jnp.float32)
        for i in range(H):
            w = jnp.broadcast_to(weight[i : i + 1, 0:1], (24, hi - lo))
            v += w * (occ_h[i, :, lo:hi] + block_mixing * occ_r[i, :, lo:hi])
        occ_out[:, lo:hi] = mask[:, lo:hi] * v

    for c, chunk in enumerate(CHUNKS):
        g0, n = chunk[0], len(chunk)
        width = slice(0, 128 * n)
        arrive(phase(c, 1), zin.at[pl.ds(g0 * NY, n * NY)])

        def z_pack(z):
            at = pl.ds(pl.multiple_of(z * 64, 64), 64)
            for g in range(n):
                lanes = slice(128 * g, 128 * g + 128)
                lines = [
                    zin[pl.ds(g0 * NY + ky * n + g, SLABS, stride=KY * n), :] for ky in range(KY)
                ]
                zh[at, lanes], zl[at, lanes] = split(regroup(lines, z))

        repeat(ZL, z_pack)
        zu[:, width] = dot3(tz0[...], tz1[...], zh[:, width], zl[:, width])

        def z_filter(z):
            at = pl.ds(pl.multiple_of(z * 64, 64), 64)
            v = zu[at, width] * fac[at, 128 * g0 : 128 * (g0 + n)]
            zh[at, width], zl[at, width] = split(v)

        repeat(ZL, z_filter)
        zu[:, width] = dot3(tz2[...], tz3[...], zh[:, width], zl[:, width])

        def z_unpack(ky):
            for g in range(n):
                lanes = slice(128 * g, 128 * g + 128)
                planes = [zu[64 * z : 64 * z + 64, lanes] for z in range(ZL)]
                at = pl.ds(g0 * NY + ky * n + g, SLABS, stride=KY * n)
                zout[at, :] = regroup(planes, ky)

        repeat(KY, z_unpack)
        done.append(
            exchange(
                phase(c, 2),
                lambda q, g0=g0, n=n: zout_rows.at[pl.ds(g0 * NY + q * (KY * n), KY * n)],
                lambda m, g0=g0, n=n: yb_rows.at[pl.ds(g0 * NY + m * (KY * n), KY * n)],
                me_s, slab_each, zout_rows.at[pl.ds(g0 * NY, (NY - KY) * n)],
            )
        )

    for c, chunk in enumerate(CHUNKS):
        g0, n = chunk[0], len(chunk)
        arrive(phase(c, 2), yb.at[pl.ds(g0 * NY, n * NY)])
        y = [yb[pl.ds(g0 * NY + g, NY, stride=n), :] for g in range(n)]
        y = jnp.concatenate(y, axis=1)
        y = dot3(tx2[...], tx3[...], *split(y))
        for g in chunk:
            lanes = slice(128 * (g - g0), 128 * (g - g0) + 128)
            yo[:, g] = y[:, lanes].reshape(PENCILS, YL, 128)
        done.append(
            exchange(
                phase(c, 3),
                lambda q, g0=g0, n=n: yo.at[q, pl.ds(g0, n)],
                lambda m, g0=g0, n=n: xi.at[m, pl.ds(g0, n)],
                me_p, pencil_each, yo.at[pl.ds(0, PENCILS - 1), pl.ds(g0, n)],
            )
        )

    for c, chunk in enumerate(CHUNKS):
        g0, g1 = chunk[0], chunk[-1] + 1
        n = g1 - g0
        rows = slice(64 * g0, 64 * g1)
        arrive(phase(c, 3), xi.at[:, pl.ds(g0, n)])
        if c == len(CHUNKS) - 1:
            break

        def end_step(z):
            at = pl.ds(pl.multiple_of(z * YL, YL), YL)
            h = regroup([xi[b, g] for g in chunk for b in range(PENCILS)], z)
            hh, hl = split(h[:, : 64 * n])
            dm[at, :] += grid_mixing * dot3(hh, hl, tx0[rows, :], tx1[rows, :])

        repeat(ZL, end_step)
        if c == len(CHUNKS) - 2:
            part = pltpu.make_async_copy(dm, part_out, load_sem.at[ZL + 1])
            part.start()
    last = pltpu.make_async_copy(xi.at[:, pl.ds(g0, n)], last_out, load_sem.at[ZL + 2])
    last.start()
    for finish in done:
        finish()
    part.wait()
    last.wait()


def last_kernel(part, last, tx0, tx1, occ, out, occ_out):
    n = last.shape[1]
    rows = slice(NX - 64 * n, NX)

    def plane_step(plane):
        at = pl.ds(pl.multiple_of(plane * YL, YL), YL)
        z = 4 * pl.program_id(0) + plane
        h = regroup([last[b, g] for g in range(n) for b in range(PENCILS)], z)
        hh, hl = split(h[:, : 64 * n])
        out[at, :] = part[at, :] + grid_mixing * dot3(hh, hl, tx0[rows, :], tx1[rows, :])

    repeat(4, plane_step)

    @pl.when(pl.program_id(0) == 0)
    def _():
        occ_out[...] = occ[...]


def body(
    density_history, residual_history, occupancy_history, occupancy_residual, species, slot_count
):
    qx = real_basis(NX)
    qz = real_basis(NZ)
    qz = qz.reshape(NZ, SLABS, ZL).transpose(0, 2, 1).reshape(NZ, NZ)
    tables = two_parts(qx) + two_parts(qx.T) + two_parts(qz) + two_parts(qz.T)
    f32 = jnp.float32
    bf16 = jnp.bfloat16
    vmem = pl.BlockSpec(memory_space=pltpu.VMEM)
    hbm = pl.BlockSpec(memory_space=pl.ANY)
    smem = pl.BlockSpec(memory_space=pltpu.SMEM)
    slots, entries = occupancy_history.shape[1:]
    rows = ZL * YL
    last_tiles = len(CHUNKS[-1])
    part, last, occupancy = pl.pallas_call(
        kernel,
        in_specs=[smem, smem] + [hbm] * 12,
        out_specs=[hbm, hbm, vmem],
        out_shape=[
            jax.ShapeDtypeStruct((rows, NX), f32),
            jax.ShapeDtypeStruct((PENCILS, last_tiles, YL, 128), f32),
            jax.ShapeDtypeStruct((slots, entries), f32),
        ],
        scratch_shapes=[
            pltpu.VMEM((H, slots, entries), f32),
            pltpu.VMEM((H, slots, entries), f32),
            pltpu.VMEM((slots, 384), f32),
            pltpu.VMEM((H, rows, NX), f32),
            pltpu.VMEM((H, rows, NX), f32),
        ]
        + [pltpu.VMEM((NX, NX), bf16)] * 4
        + [pltpu.VMEM((NZ, NZ), bf16)] * 4
        + [
            pltpu.VMEM((1, 1, 128), f32),
            pltpu.VMEM((EIGHT, 1, 128), f32),
            pltpu.VMEM((1, 1, 128), f32),
            pltpu.VMEM((SLABS // 2, 1, 128), f32),
            pltpu.VMEM((8, 128), f32),
            pltpu.VMEM((rows, NX), bf16),
            pltpu.VMEM((rows, NX), bf16),
            pltpu.VMEM((rows, 128 * len(CHUNKS)), f32),
            pltpu.VMEM((PENCILS, LT, YL, 128), f32),
            pltpu.VMEM((PENCILS, LT, YL, 128), f32),
            pltpu.VMEM((LT * NY, 128), f32),
            pltpu.VMEM((LT * NY, 128), f32),
            pltpu.VMEM((NZ, 256), bf16),
            pltpu.VMEM((NZ, 256), bf16),
            pltpu.VMEM((NZ, 128 * LT), f32),
            pltpu.VMEM((NZ, 256), f32),
            pltpu.VMEM((LT * NY, 128), f32),
            pltpu.VMEM((LT * NY, 128), f32),
            pltpu.VMEM((PENCILS, LT, YL, 128), f32),
            pltpu.VMEM((PENCILS, LT, YL, 128), f32),
            pltpu.VMEM((rows, NX), f32),
            pltpu.SemaphoreType.DMA((ZL + 3,)),
            pltpu.SemaphoreType.DMA((10,)),
            pltpu.SemaphoreType.DMA((2 + 4 * len(CHUNKS),)),
            pltpu.SemaphoreType.DMA((2 + 4 * len(CHUNKS),)),
        ],
        compiler_params=pltpu.CompilerParams(
            collective_id=0, has_side_effects=True, vmem_limit_bytes=56 * 2**20
        ),
    )(
        species,
        slot_count,
        residual_history.reshape(H, rows, NX),
        density_history.reshape(H, rows, NX),
        occupancy_history,
        occupancy_residual,
        *tables,
    )
    new_density, new_occupancy = pl.pallas_call(
        last_kernel,
        grid=(ZL // 4,),
        in_specs=[
            pl.BlockSpec((4 * YL, NX), lambda z: (z, 0)),
            pl.BlockSpec(last.shape, lambda z: (0, 0, 0, 0)),
            pl.BlockSpec((NX, NX), lambda z: (0, 0)),
            pl.BlockSpec((NX, NX), lambda z: (0, 0)),
            pl.BlockSpec((slots, entries), lambda z: (0, 0)),
        ],
        out_specs=[
            pl.BlockSpec((4 * YL, NX), lambda z: (z, 0)),
            pl.BlockSpec((slots, entries), lambda z: (0, 0)),
        ],
        out_shape=[
            jax.ShapeDtypeStruct((rows, NX), f32),
            jax.ShapeDtypeStruct((slots, entries), f32),
        ],
    )(part, last, tables[0], tables[1], occupancy)
    return (new_density.reshape(ZL, YL, NX), new_occupancy)


def solution(mesh):
    torus = Mesh(
        mesh.devices.reshape(8, 4, 2, mesh.shape["pencil"]),
        ("slab_0", "slab_1", "slab_2", "pencil"),
    )
    placed = (
        P(None, SLAB, "pencil", None),
        P(None, SLAB, "pencil", None),
        P(None, SLAB_PENCIL, None),
        P(None, SLAB_PENCIL, None),
        P(SLAB_PENCIL),
        P(SLAB_PENCIL),
    )
    return jax.shard_map(
        body,
        mesh=torus,
        in_specs=placed,
        out_specs=(P(SLAB, "pencil", None), P(SLAB_PENCIL, None)),
        check_vma=False,
    )
```
